32 devices in a mesh: dev: 32 (over z, y, x, core).
Axes of the slice: x: 2, y: 2, z: 4, core: 2. Of those that a mesh axis runs over, the one named last changes fastest.
Arguments:
- tokens: bfloat16 [576, 197, 384], P('dev'), may hold values from -6 to 6
- cotangent: bfloat16 [576, 197, 384], P('dev'), may hold values from -6 to 6
- valid_slots: int32 [576], P('dev'), may hold values from 0 to 1, as said below
- qkv_weight: bfloat16 [442368], P('dev'), may hold values from -0.3125 to 0.3125
- out_weight: bfloat16 [147456], P('dev'), may hold values from -1.25 to 1.25
- fc1_weight: bfloat16 [589824], P('dev'), may hold values from -0.3125 to 0.3125
- fc2_weight: bfloat16 [589824], P('dev'), may hold values from -0.15625 to 0.15625
- norm_params: bfloat16 [1536], P('dev'), may hold values from -2 to 2
- bias_params: bfloat16 [3072], P('dev'), may hold values from -3 to 3
Outputs:
- block_output: bfloat16 [576, 197, 384], P('dev')
- input_grad: float32 [576, 197, 384], P('dev')
- qkv_grad: float32 [442368], P('dev')
- out_grad: float32 [147456], P('dev')
- fc1_grad: float32 [589824], P('dev')
- fc2_grad: float32 [589824], P('dev')
- norm_grad: float32 [1536], P('dev')
- bias_grad: float32 [3072], P('dev')
The draws below stay inside these ranges and needn't reach their ends.
Inputs may be any that keep to these rules, and one draw needn't show every extreme that they name: `valid_slots`: each device's 18 slots hold 18 or 17 images; in every draw some devices hold 18 and some 18 - 1.
All inputs are finite; a program needn't handle non-finite values.
Results may differ from the reference program's by a relative error of at most 0.011.
Values may be sent and summed in bfloat16 or wider, within the bound.
A program may use at most 320 MiB of HBM per device.

```python
import jax
import jax.numpy as jnp
from jax import lax

D = 384
HEADS = 6
HEAD_DIM = 64
FF = 1536
SEQ = 197
IMG_DEV = 18
SLOTS = 576


def draw_valid_slots(key, part):
    devices = SLOTS // IMG_DEV
    key_full, key_order, key_place = jax.random.split(key, 3)
    full_count = jax.random.randint(key_full, (), 1, devices)
    order = jax.random.permutation(key_order, devices)
    empty_at = jax.random.randint(key_place, (devices,), 0, IMG_DEV)
    slot_index = jnp.arange(IMG_DEV, dtype=jnp.int32)
    keeps = (order < full_count)[:, None] | (slot_index[None, :] != empty_at[:, None])
    return keeps.astype(jnp.int32).reshape(SLOTS)


def draw_norm_params(key, part):
    key_gain, key_shift = jax.random.split(key)
    index = jnp.arange(4 * D)
    is_gain = (index < D) | (index >= 2 * D) & (index < 3 * D)
    gains = jax.random.uniform(key_gain, (4 * D,), jnp.float32, 0.5, 1.5)
    shifts = 0.5 * jnp.clip(jax.random.normal(key_shift, (4 * D,), jnp.float32), -4.0, 4.0)
    return jnp.where(is_gain, gains, shifts).astype(jnp.bfloat16)


def raised(entries, stream_key, source, target, shards_of, factor):
    def block_of(position):
        return (jnp.arange(entries.shape[position]) // (entries.shape[position] // shards_of)).reshape((-1,) + (1,) * (entries.ndim - 1 - position))

    first = jax.random.permutation(stream_key, shards_of)[block_of(target)]
    second = (block_of(target) + shards_of // 2) % shards_of
    return jnp.where((block_of(source) == first) | (block_of(source) == second), factor * entries, entries)


def block_levels(stream_key, shape, pieces, smallest, top_value):
    def one(position, blocks):
        steps = jax.random.uniform(jax.random.fold_in(jax.random.fold_in(stream_key, 6), position), (blocks,), jnp.float32, smallest / len(pieces), top_value / len(pieces))
        return jnp.repeat(jnp.exp(steps), shape[position] // blocks).reshape((-1,) + (1,) * (len(shape) - position - 1))

    loudness = one(*pieces[0])
    for cut in pieces[1:]:
        loudness = loudness * one(*cut)
    return loudness


def noise(rng, extent, deviation, bound, cuts=(), kind=jnp.bfloat16):
    level = block_levels(rng, extent, cuts, -0.22, 0.18) if cuts else 1.0
    values = jax.random.normal(rng, extent, jnp.float32) * deviation * level
    return jnp.minimum(jnp.maximum(values, -bound), bound).astype(kind)


def noise_with(stream_key, shape, spread, reach, cuts, heavy, held_as=jnp.bfloat16):
    entries = spread * jax.random.normal(stream_key, shape, jnp.float32)
    if cuts:
        entries = entries * block_levels(stream_key, shape, cuts, -0.22, 0.18)
    return jnp.clip(raised(entries, jax.random.fold_in(stream_key, 3), *heavy), -reach, reach).astype(held_as)


def setup_inputs(seed: int = 0) -> dict:
    splits = jax.random.split(jax.random.key(seed), 10)
    tokens = noise(splits[0], (SLOTS, SEQ, D), 1.0, 6.0, ((0, 32),))
    cotangent = noise_with(splits[1], (SLOTS, SEQ, D), 1.0, 6.0, ((0, 32),), (0, 2, 32, 2.75))
    valid_slots = draw_valid_slots(jax.random.fold_in(splits[9], 71), 0)
    qkv_weight = noise(splits[3], (3 * D * D,), D ** -0.5, 0.3125, ((0, 32),))
    out_weight = noise(splits[4], (D * D,), (D // 16) ** -0.5, 1.25, ((0, 32),))
    fc1_weight = noise(splits[5], (D * FF,), D ** -0.5, 0.3125, ((0, 32),))
    fc2_weight = noise(splits[6], (FF * D,), FF ** -0.5, 0.15625, ((0, 32),))
    norm_params = draw_norm_params(jax.random.fold_in(splits[9], 71), 0)
    bias_params = noise(splits[8], (4 * D + FF,), 0.5, 3.0, ((0, 32),))
    return dict(tokens=tokens, cotangent=cotangent, valid_slots=valid_slots, qkv_weight=qkv_weight, out_weight=out_weight, fc1_weight=fc1_weight, fc2_weight=fc2_weight, norm_params=norm_params, bias_params=bias_params)


@jax.custom_vjp
def low(v):
    return lax.optimization_barrier(v.astype(jnp.bfloat16)).astype(jnp.float32)

@jax.custom_vjp
def low_back(v):
    return v

def low_keep(v):
    return (low(v), None)

def low_pass(kept, grad):
    return (grad,)

def back_keep(v):
    return (v, None)

def back_low(kept, grad):
    return (low(grad),)
low.defvjp(low_keep, low_pass)
low_back.defvjp(back_keep, back_low)

def highest(left, right):
    return jnp.dot(left, right, precision=lax.Precision.HIGHEST, preferred_element_type=jnp.float32)

def normalize(value, gain, shift):
    mean = lax.optimization_barrier(jnp.mean(value, axis=-1, keepdims=True))
    centered = value - mean
    inverse = lax.rsqrt(lax.optimization_barrier(jnp.mean(centered * centered, axis=-1, keepdims=True)) + 1e-06)
    return centered * inverse * gain + shift

def block(inputs, slot_mask, qkv_full, out_full, fc1_full, fc2_full, norm_full, bias_full):
    images = inputs.shape[0]
    rows = inputs.reshape(images * SEQ, D)
    normed_one = low(normalize(rows, norm_full[:D], norm_full[D:2 * D]))
    projected = low_back(highest(normed_one, qkv_full))
    queries = low(projected[:, :D] + bias_full[:D]).reshape(images, SEQ, HEADS, HEAD_DIM)
    keys_low = low(projected[:, D:2 * D]).reshape(images, SEQ, HEADS, HEAD_DIM)
    values_low = low(projected[:, 2 * D:] + bias_full[D:2 * D]).reshape(images, SEQ, HEADS, HEAD_DIM)
    scores = low_back(jnp.einsum('bqhd,bkhd->bhqk', queries, keys_low, precision=lax.Precision.HIGHEST) * HEAD_DIM ** (-0.5))
    weights_low = low(jax.nn.softmax(scores, axis=-1))
    mixed = jnp.einsum('bhqk,bkhd->bqhd', weights_low, values_low, precision=lax.Precision.HIGHEST)
    mixed_low = low(low_back(mixed)).reshape(images * SEQ, D)
    residual = rows + low_back(highest(mixed_low, out_full)) + bias_full[2 * D:3 * D]
    normed_two = low(normalize(residual, norm_full[2 * D:3 * D], norm_full[3 * D:]))
    hidden_pre = low_back(highest(normed_two, fc1_full)) + bias_full[3 * D:3 * D + FF]
    hidden_low = low(jax.nn.gelu(hidden_pre, approximate=False))
    result = residual + low_back(highest(hidden_low, fc2_full)) + bias_full[3 * D + FF:]
    return result.reshape(images, SEQ, D) * slot_mask[:, None, None]

def reference(tokens, cotangent, valid_slots, qkv_weight, out_weight, fc1_weight, fc2_weight, norm_params, bias_params):
    slot_mask = valid_slots.astype(jnp.float32)
    groups = SLOTS // IMG_DEV

    def forward(inputs, qkv_full, out_full, fc1_full, fc2_full, norm_full, bias_full):
        grouped = inputs.reshape(groups, IMG_DEV, SEQ, D)
        masks = slot_mask.reshape(groups, IMG_DEV)

        def one_group(item):
            return block(item[0], item[1], qkv_full, out_full, fc1_full, fc2_full, norm_full, bias_full)
        result = lax.map(jax.checkpoint(one_group), (grouped, masks))
        return result.reshape(SLOTS, SEQ, D)
    outputs, pull = jax.vjp(forward, tokens.astype(jnp.float32), qkv_weight.astype(jnp.float32).reshape(D, 3 * D), out_weight.astype(jnp.float32).reshape(D, D), fc1_weight.astype(jnp.float32).reshape(D, FF), fc2_weight.astype(jnp.float32).reshape(FF, D), norm_params.astype(jnp.float32), bias_params.astype(jnp.float32))
    grads = pull(cotangent.astype(jnp.float32))
    return (outputs.astype(jnp.bfloat16), grads[0], grads[1].reshape(-1), grads[2].reshape(-1), grads[3].reshape(-1), grads[4].reshape(-1), grads[5], grads[6])
```

```python
import functools
import jax
import jax.numpy as jnp
from jax import lax
from jax.experimental import pallas as pl
from jax.experimental.pallas import tpu as pltpu
from jax.sharding import PartitionSpec as P

D, HEADS, HEAD_DIM, FF = 384, 6, 64, 1536
EPS = 1e-6
F32, BF16 = jnp.float32, jnp.bfloat16
RS2 = 0.7071067811865476
RS2PI = 0.3989422804014327
VM = pltpu.VMEM


def nn(a, b):
    return lax.dot_general(a, b, (((1,), (0,)), ((), ())), preferred_element_type=F32)


def nt(a, b):
    return lax.dot_general(a, b, (((1,), (1,)), ((), ())), preferred_element_type=F32)


def tn(a, b):
    return lax.dot_general(a, b, (((0,), (0,)), ((), ())), preferred_element_type=F32)


def col8(v):
    return v.reshape(v.shape[0] // 8, 8, v.shape[1]).sum(axis=0)


def norm_fwd(v):
    c = v - jnp.mean(v, axis=1, keepdims=True)
    r = lax.rsqrt(jnp.mean(c * c, axis=1, keepdims=True) + EPS)
    return c * r, r


def norm_bwd(g, n, r, gain):
    e = g * gain
    return r * (e - jnp.mean(e, axis=1, keepdims=True) - n * jnp.mean(e * n, axis=1, keepdims=True))


def fused_kernel(L, LP, QP, CH, valid, x_ref, c_ref, wqkv, wo, w1, w2, nrm, bia, bhid,
                 out_ref, dx_ref, gqkv, gout, gfc1, gfc2, gsm,
                 xp, cp, n1s, r1s, h1s, qs, ks, vs, ps, os_, x1s, n2s, h2s, as_, gzs, gos, gts):
    i = pl.program_id(0)

    @pl.when(i == 0)
    def _():
        for r in (gqkv, gout, gfc1, gfc2, gsm):
            r[...] = jnp.zeros_like(r)
        xp[...] = jnp.zeros_like(xp)
        cp[...] = jnp.zeros_like(cp)
        qs[...] = jnp.zeros_like(qs)
        gos[...] = jnp.zeros_like(gos)

    mask = valid[i].astype(F32)
    g1, c1, g2, c2 = (nrm[j:j + 1, :] for j in range(4))
    bq, bv, bo, b2 = (bia[j:j + 1, :] for j in range(4))
    lane = lax.broadcasted_iota(jnp.int32, (1, 128), 1)
    low = lane < 64

    xp[:L, :] = x_ref[0]
    cp[:L, :] = c_ref[0]

    def stacked(ref, cols):
        v = ref[:, cols]
        z = jnp.zeros_like(v)
        return jnp.concatenate([jnp.where(low, v, z), jnp.where(low, z, v)], axis=0)

    n1, r1 = norm_fwd(xp[...].astype(F32))
    n1s[...] = n1
    r1s[...] = r1
    h1s[...] = (n1 * g1 + c1).astype(BF16)
    t = nn(h1s[...], wqkv[...])
    qs[:LP, :] = (t[:, :D] + bq).astype(BF16) * BF16(0.125)
    ks[...] = t[:, D:2 * D].astype(BF16)
    vs[...] = (t[:, 2 * D:] + bv).astype(BF16)
    for j in range(HEADS // 2):
        cols = slice(128 * j, 128 * j + 128)
        st = nt(ks[:, cols], stacked(qs, cols))
        top, bot = st[:LP - 16], st[LP - 16:]
        row = lax.broadcasted_iota(jnp.int32, bot.shape, 0) + (LP - 16)
        bot = jnp.where(row < L, bot, -1e30)
        mx = jnp.maximum(jnp.max(top, axis=0, keepdims=True), jnp.max(bot, axis=0, keepdims=True))
        e = jnp.exp(jnp.concatenate([top, bot], axis=0) - mx)
        p = e * (1.0 / jnp.sum(e, axis=0, keepdims=True))
        ps[j] = p.astype(BF16)
        o2 = tn(ps[j], vs[:, cols])
        os_[:, cols] = jnp.where(low, o2[:LP], o2[QP:QP + LP]).astype(BF16)
    x1 = xp[...].astype(F32) + nn(os_[...], wo[...]) + bo
    x1s[...] = x1
    n2, r2 = norm_fwd(x1)
    n2s[...] = n2
    h2s[...] = (n2 * g2 + c2).astype(BF16)

    gyb = cp[...] * mask.astype(BF16)
    for c in range(FF // CH):
        cols = slice(c * CH, (c + 1) * CH)
        z = nn(h2s[...], w1[:, cols]) + bhid[:, cols]
        ga = nt(gyb, w2[cols, :])
        phi = 0.5 + 0.5 * lax.erf(z * RS2)
        as_[:, cols] = (z * phi).astype(BF16)
        gz = ga * (phi + z * (RS2PI * jnp.exp(-0.5 * z * z)))
        gsm[:, 7 * D + c * CH:7 * D + (c + 1) * CH] += col8(gz)
        gzs[:, cols] = gz.astype(BF16)
    y = (x1s[...] + nn(as_[...], w2[...]) + b2) * mask
    out_ref[0] = y[:L].astype(BF16)
    gfc2[...] += tn(as_[...], gyb)
    gfc1[...] += tn(h2s[...], gzs[...])
    gh2 = nt(gzs[...], w1[...])
    n2 = n2s[...]
    gy = gyb.astype(F32)
    gsm[:, 2 * D:3 * D] += col8(gh2 * n2)
    gsm[:, 3 * D:4 * D] += col8(gh2)
    gsm[:, 7 * D + FF:] += col8(gy)
    gx1 = gy + norm_bwd(gh2, n2, r2, g2)
    x1s[...] = gx1
    gsm[:, 6 * D:7 * D] += col8(gx1)
    gx1b = gx1.astype(BF16)
    gout[...] += tn(os_[...], gx1b)
    gos[:LP, :] = nt(gx1b, wo[...]).astype(BF16)

    for j in range(HEADS // 2):
        cols = slice(128 * j, 128 * j + 128)
        p = ps[j]
        gv = jnp.where(low, nn(p[:, :QP], gos[:, cols]), nn(p[:, QP:], gos[:, cols]))
        gp = nt(vs[:, cols], stacked(gos, cols))
        pf = p.astype(F32)
        gs = (pf * (gp - jnp.sum(gp * pf, axis=0, keepdims=True))).astype(BF16)
        q2 = tn(gs, ks[:, cols])
        gq = jnp.where(low, q2[:LP], q2[QP:QP + LP]) * 0.125
        gk = jnp.where(low, nn(gs[:, :QP], qs[:, cols]), nn(gs[:, QP:], qs[:, cols]))
        gsm[:, 4 * D + 128 * j:4 * D + 128 * j + 128] += col8(gq)
        gsm[:, 5 * D + 128 * j:5 * D + 128 * j + 128] += col8(gv)
        gts[:, 128 * j:128 * j + 128] = gq.astype(BF16)
        gts[:, D + 128 * j:D + 128 * j + 128] = gk.astype(BF16)
        gts[:, 2 * D + 128 * j:2 * D + 128 * j + 128] = gv.astype(BF16)
    gqkv[...] += tn(h1s[...], gts[...])
    gh1 = nt(gts[...], wqkv[...])
    n1 = n1s[...]
    gsm[:, :D] += col8(gh1 * n1)
    gsm[:, D:2 * D] += col8(gh1)
    dx = x1s[...] + norm_bwd(gh1, n1, r1s[...], g1)
    dx_ref[0] = dx[:L]


def fused(tokens, cot, valid, wqkv, wo, w1, w2, nrm, bia, bhid):
    N, L, _ = tokens.shape
    LP = -(-L // 16) * 16
    QP = -(-L // 128) * 128
    const = lambda *s: pl.BlockSpec(s, lambda i, v: (0,) * len(s), pipeline_mode=pl.Buffered(1))
    img = lambda: pl.BlockSpec((1, L, D), lambda i, v: (i, 0, 0))
    grid_spec = pltpu.PrefetchScalarGridSpec(
        num_scalar_prefetch=1, grid=(N,),
        in_specs=[img(), img(), const(D, 3 * D), const(D, D), const(D, FF), const(FF, D),
                  const(4, D), const(4, D), const(1, FF)],
        out_specs=[img(), img(), const(D, 3 * D), const(D, D), const(D, FF), const(FF, D), const(8, 8 * D + FF)],
        scratch_shapes=[
            VM((LP, D), BF16), VM((LP, D), BF16), VM((LP, D), F32), VM((LP, 1), F32), VM((LP, D), BF16),
            VM((QP, D), BF16), VM((LP, D), BF16), VM((LP, D), BF16), VM((HEADS // 2, LP, 2 * QP), BF16),
            VM((LP, D), BF16), VM((LP, D), F32), VM((LP, D), F32), VM((LP, D), BF16),
            VM((LP, FF), BF16), VM((LP, FF), BF16), VM((QP, D), BF16), VM((LP, 3 * D), BF16)])
    sds = jax.ShapeDtypeStruct
    return pl.pallas_call(
        functools.partial(fused_kernel, L, LP, QP, 512),
        grid_spec=grid_spec,
        out_shape=[sds((N, L, D), BF16), sds((N, L, D), F32), sds((D, 3 * D), F32), sds((D, D), F32),
                   sds((D, FF), F32), sds((FF, D), F32), sds((8, 8 * D + FF), F32)],
        compiler_params=pltpu.CompilerParams(vmem_limit_bytes=60 << 20),
    )(valid, tokens, cot, wqkv, wo, w1, w2, nrm, bia, bhid)


def local(tokens, cotangent, valid_slots, qkv_weight, out_weight, fc1_weight, fc2_weight, norm_params, bias_params):
    ag = lambda v: lax.all_gather(v, "dev", axis=0, tiled=True)
    rs = lambda v: lax.psum_scatter(v, "dev", scatter_dimension=0, tiled=True)
    wqkv = ag(qkv_weight).reshape(D, 3 * D)
    wo = ag(out_weight).reshape(D, D)
    w1 = ag(fc1_weight).reshape(D, FF)
    w2 = ag(fc2_weight).reshape(FF, D)
    nrm = ag(norm_params).astype(F32).reshape(4, D)
    b = ag(bias_params).astype(F32)
    bia = jnp.concatenate([b[:3 * D], b[3 * D + FF:]]).reshape(4, D)
    bhid = b[3 * D:3 * D + FF].reshape(1, FF)
    out, dx, gqkv, gout, gfc1, gfc2, gsm = fused(tokens, cotangent, valid_slots, wqkv, wo, w1, w2, nrm, bia, bhid)
    gsm = jnp.sum(gsm, axis=0)
    return (out, dx, rs(gqkv.reshape(-1)), rs(gout.reshape(-1)), rs(gfc1.reshape(-1)), rs(gfc2.reshape(-1)),
            rs(gsm[:4 * D]), rs(gsm[4 * D:]))


def solution(mesh):
    s3, s1 = P("dev", None, None), P("dev")
    return jax.shard_map(local, mesh=mesh, in_specs=(s3, s3) + (s1,) * 7, out_specs=(s3, s3) + (s1,) * 6, check_vma=False)
```

```python
import functools
import jax
import jax.numpy as jnp
from jax import lax
from jax.experimental import pallas as pl
from jax.experimental.pallas import tpu as pltpu
from jax.sharding import PartitionSpec as P

D, HEADS, HEAD_DIM, FF = 384, 6, 64, 1536
PAIRS = HEADS // 2
EPS = 1e-6
F32, BF16 = jnp.float32, jnp.bfloat16
RS2 = 0.7071067811865476
RS2PI = 0.3989422804014327
VM = pltpu.VMEM
BIAS_ROW = 16
SDS = jax.ShapeDtypeStruct


def nn(a, b):
    return lax.dot_general(a, b, (((1,), (0,)), ((), ())), preferred_element_type=F32)


def nt(a, b):
    return lax.dot_general(a, b, (((1,), (1,)), ((), ())), preferred_element_type=F32)


def tn(a, b):
    return lax.dot_general(a, b, (((0,), (0,)), ((), ())), preferred_element_type=F32)


def col8(v):
    return v.reshape(v.shape[0] // 8, 8, v.shape[1]).sum(axis=0)


def norm_fwd(v):
    c = v - jnp.mean(v, axis=1, keepdims=True)
    r = lax.rsqrt(jnp.mean(c * c, axis=1, keepdims=True) + EPS)
    return c * r, r


def norm_bwd(g, n, r, gain):
    e = g * gain
    return r * (e - jnp.mean(e, axis=1, keepdims=True) - n * jnp.mean(e * n, axis=1, keepdims=True))


def vec(sml, row, count=3):
    return jnp.concatenate([sml[row + j:row + j + 1, :] for j in range(count)], axis=1)


def low_lanes():
    return lax.broadcasted_iota(jnp.int32, (1, 128), 1) < 64


def stacked(v):
    low, z = low_lanes(), jnp.zeros_like(v)
    return jnp.concatenate([jnp.where(low, v, z), jnp.where(low, z, v)], axis=0)


class Pad:
    def __init__(self, tokens):
        self.n, self.len, _ = tokens.shape
        self.rows = -(-self.len // 16) * 16
        self.lanes = -(-self.len // 128) * 128

    def step(self, most):
        return max(b for b in range(1, most + 1) if self.n % b == 0)


def attn_fwd(s, b, x_ref, wqkv, sml, q_ref, k_ref, v_ref, p_ref, o_ref, xp, h1, ks, vs):
    lp, qp, low = s.rows, s.lanes, low_lanes()
    for u in range(b):
        xp[u * lp:u * lp + s.len, :] = x_ref[u]
    n1, _ = norm_fwd(xp[...].astype(F32))
    h1[...] = (n1 * vec(sml, 0) + vec(sml, 3)).astype(BF16)
    t = nn(h1[...], wqkv[...])
    q = (t[:, :D] + vec(sml, BIAS_ROW)).astype(BF16) * BF16(0.125)
    k = t[:, D:2 * D].astype(BF16)
    v = (t[:, 2 * D:] + vec(sml, BIAS_ROW + 3)).astype(BF16)
    for u in range(b):
        rows = slice(u * lp, u * lp + lp)
        q_ref[u, :lp, :] = q[rows]
        q_ref[u, lp:, :] = jnp.zeros((qp - lp, D), BF16)
        k_ref[u] = k[rows]
        v_ref[u] = v[rows]
    for u in range(b):
        for j in range(PAIRS):
            cols = slice(128 * j, 128 * j + 128)
            st = nt(k_ref[u, :, cols], stacked(q_ref[u, :, cols]))
            top, bot = st[:lp - 16], st[lp - 16:]
            row = lax.broadcasted_iota(jnp.int32, bot.shape, 0) + (lp - 16)
            bot = jnp.where(row < s.len, bot, -1e30)
            mx = jnp.maximum(jnp.max(top, axis=0, keepdims=True), jnp.max(bot, axis=0, keepdims=True))
            e = jnp.exp(jnp.concatenate([top, bot], axis=0) - mx)
            p = e * (1.0 / jnp.sum(e, axis=0, keepdims=True))
            p_ref[u, j] = p.astype(BF16)
            o2 = tn(p_ref[u, j], v_ref[u, :, cols])
            o_ref[u, :, cols] = jnp.where(low, o2[:lp], o2[qp:qp + lp]).astype(BF16)


def ffn(s, b, ch, i, valid, x_ref, c_ref, o_ref, wo, w1, w2, sml,
        out_ref, gx_ref, go_ref, gout, gfc1, gfc2, gsm, xp, cp, os_, n2s, h2s, as_, gzs, x1s):
    lp, qp = s.rows, s.lanes
    g2, c2 = vec(sml, 6), vec(sml, 9)
    bo, bh, b2 = vec(sml, BIAS_ROW + 6), vec(sml, BIAS_ROW + 9, 12), vec(sml, BIAS_ROW + 21)
    for u in range(b):
        xp[u * lp:u * lp + s.len, :] = x_ref[u]
        cp[u * lp:u * lp + s.len, :] = c_ref[u] * valid[i * b + u].astype(BF16)
        os_[u * lp:u * lp + lp, :] = o_ref[u]
    x1 = xp[...].astype(F32) + nn(os_[...], wo[...]) + bo
    x1s[...] = x1
    n2, r2 = norm_fwd(x1)
    n2s[...] = n2
    h2s[...] = (n2 * g2 + c2).astype(BF16)
    for c in range(FF // ch):
        cols = slice(c * ch, (c + 1) * ch)
        z = nn(h2s[...], w1[:, cols]) + bh[:, cols]
        ga = nt(cp[...], w2[cols, :])
        phi = 0.5 + 0.5 * lax.erf(z * RS2)
        as_[:, cols] = (z * phi).astype(BF16)
        gz = ga * (phi + z * (RS2PI * jnp.exp(-0.5 * z * z)))
        gsm[:, 7 * D + c * ch:7 * D + (c + 1) * ch] += col8(gz)
        gzs[:, cols] = gz.astype(BF16)
    y = x1s[...] + nn(as_[...], w2[...]) + b2
    for u in range(b):
        out_ref[u] = (y[u * lp:u * lp + s.len] * valid[i * b + u].astype(F32)).astype(BF16)
    gfc2[...] += tn(as_[...], cp[...])
    gfc1[...] += tn(h2s[...], gzs[...])
    gh2 = nt(gzs[...], w1[...])
    n2 = n2s[...]
    gy = cp[...].astype(F32)
    gsm[:, 2 * D:3 * D] += col8(gh2 * n2)
    gsm[:, 3 * D:4 * D] += col8(gh2)
    gsm[:, 7 * D + FF:] += col8(gy)
    gx1 = gy + norm_bwd(gh2, n2, r2, g2)
    gsm[:, 6 * D:7 * D] += col8(gx1)
    gx1b = gx1.astype(BF16)
    gout[...] += tn(os_[...], gx1b)
    go = nt(gx1b, wo[...]).astype(BF16)
    for u in range(b):
        gx_ref[u] = gx1[u * lp:u * lp + lp]
        go_ref[u, :lp, :] = go[u * lp:u * lp + lp]
        go_ref[u, lp:, :] = jnp.zeros((qp - lp, D), BF16)


def attn_bwd(s, b, q_ref, k_ref, v_ref, p_ref, go_ref, gt_ref, gqv):
    lp, qp, low = s.rows, s.lanes, low_lanes()
    for u in range(b):
        for j in range(PAIRS):
            cols = slice(128 * j, 128 * j + 128)
            p, go = p_ref[u, j], go_ref[u, :, cols]
            gv = jnp.where(low, nn(p[:, :qp], go), nn(p[:, qp:], go))
            gp = nt(v_ref[u, :, cols], stacked(go))
            pf = p.astype(F32)
            gs = (pf * (gp - jnp.sum(gp * pf, axis=0, keepdims=True))).astype(BF16)
            q2 = tn(gs, k_ref[u, :, cols])
            gq = jnp.where(low, q2[:lp], q2[qp:qp + lp]) * 0.125
            q = q_ref[u, :, cols]
            gk = jnp.where(low, nn(gs[:, :qp], q), nn(gs[:, qp:], q))
            gqv[:, 128 * j:128 * j + 128] += col8(gq)
            gqv[:, D + 128 * j:D + 128 * j + 128] += col8(gv)
            gt_ref[u, :, 128 * j:128 * j + 128] = gq.astype(BF16)
            gt_ref[u, :, D + 128 * j:D + 128 * j + 128] = gk.astype(BF16)
            gt_ref[u, :, 2 * D + 128 * j:2 * D + 128 * j + 128] = gv.astype(BF16)


def proj_bwd(s, b, x_ref, gt_ref, gx_ref, wqkv, sml, dx_ref, gqkv, gn1, xp, h1, gts):
    lp = s.rows
    g1 = vec(sml, 0)
    for u in range(b):
        xp[u * lp:u * lp + s.len, :] = x_ref[u]
        gts[u * lp:u * lp + lp, :] = gt_ref[u]
    n1, r1 = norm_fwd(xp[...].astype(F32))
    h1[...] = (n1 * g1 + vec(sml, 3)).astype(BF16)
    gqkv[...] += tn(h1[...], gts[...])
    gh1 = nt(gts[...], wqkv[...])
    gn1[:, :D] += col8(gh1 * n1)
    gn1[:, D:] += col8(gh1)
    back = norm_bwd(gh1, n1, r1, g1)
    for u in range(b):
        dx_ref[u] = gx_ref[u, :s.len] + back[u * lp:u * lp + s.len]


def zero(*refs):
    for r in refs:
        r[...] = jnp.zeros_like(r)


def img(b, *shape):
    return pl.BlockSpec((b,) + shape, lambda i, *_: (i,) + (0,) * len(shape))


def const(*shape):
    return pl.BlockSpec(shape, lambda i, *_: (0,) * len(shape), pipeline_mode=pl.Buffered(1))


def big(**kw):
    return pltpu.CompilerParams(vmem_limit_bytes=62 << 20, **kw)


MESHID = pl.DeviceIdType.MESH


def chip_dims(n):
    chips = n // 2
    side = 4 if chips >= 64 else 2
    return (chips // (side * side), side, side)


class Place:
    def __init__(self, n):
        self.n, self.dims = n, chip_dims(n)
        me = lax.axis_index("dev")
        self.me, self.core = me, lax.rem(me, 2)
        s0, s1, s2 = self.dims
        chip = me // 2
        self.at = (chip // (s1 * s2), lax.rem(chip // s2, s1), lax.rem(chip, s2))
        self.offs = [(a, b, c) for a in range(s0) for b in range(s1) for c in range(s2)]

    def chip(self, off):
        i0, i1, i2 = (lax.rem(i + s + o, s) for i, s, o in zip(self.at, self.dims, off))
        return (i0 * self.dims[1] + i1) * self.dims[2] + i2

    def dev(self, off):
        return 2 * self.chip(off) + self.core

    def partner(self, off=(0, 0, 0)):
        return 2 * self.chip(off) + 1 - self.core

    def num(self, off):
        return (off[0] * self.dims[1] + off[1]) * self.dims[2] + off[2]

    def peers(self):
        for k in range(3):
            for o in range(1, self.dims[k]):
                yield self.dev(unit(k, o))
        yield self.partner()


def unit(k, o):
    return tuple(o if j == k else 0 for j in range(3))


def neg(off):
    return tuple(-o for o in off)


def greet(pl_):
    barrier = pltpu.get_barrier_semaphore()
    count = 0
    for dev in pl_.peers():
        pl.semaphore_signal(barrier, inc=1, device_id=(dev,), device_id_type=MESHID)
        count += 1
    pl.semaphore_wait(barrier, count)


ORDERS = ((0, 2, 1), (0, 1, 2))


class Gather:
    def __init__(self, place, src, buf, ssem, rsem):
        self.p, self.src, self.buf, self.ssem, self.rsem = place, src, buf, ssem, rsem
        self.half = src.shape[0] // 2

    def link(self, h, off, to, dev):
        p, rows = self.p, pl.ds(h * self.half, self.half)
        origin = p.dev(neg(off))
        src = self.src.at[rows] if not any(off) else self.buf.at[origin, rows]
        k = p.num(to)
        return pltpu.make_async_remote_copy(
            src_ref=src, dst_ref=self.buf.at[origin, rows], send_sem=self.ssem.at[0, h, k],
            recv_sem=self.rsem.at[0, h, k], device_id=(dev,), device_id_type=MESHID)

    def cross(self, h, off):
        p, rows = self.p, pl.ds(h * self.half, self.half)
        origin = p.dev(neg(off))
        src = self.src.at[rows] if not any(off) else self.buf.at[origin, rows]
        k = p.num(off)
        return pltpu.make_async_remote_copy(
            src_ref=src, dst_ref=self.buf.at[origin, rows], send_sem=self.ssem.at[1, h, k],
            recv_sem=self.rsem.at[1, h, k], device_id=(p.partner(),), device_id_type=MESHID)

    def hops(self, h, off):
        order = ORDERS[h]
        last = max([j for j in range(3) if off[order[j]]], default=-1)
        for j in range(last + 1, 3):
            k = order[j]
            for o in range(1, self.p.dims[k]):
                to = tuple(a + b for a, b in zip(off, unit(k, o)))
                yield to, self.p.dev(unit(k, o))

    def forward(self, h, off):
        for to, dev in self.hops(h, off):
            self.link(h, off, to, dev).start()
        self.cross(h, off).start()

    def begin(self):
        for h in range(2):
            self.forward(h, (0, 0, 0))

    def arrivals(self):
        offs = sorted([o for o in self.p.offs if any(o)], key=lambda o: (sum(1 for a in o if a), min(o[0], self.p.dims[0] - o[0])))
        return [(h, o) for o in offs for h in range(2)]

    def arrive(self, h, off):
        self.link(h, off, off, self.p.me).wait_recv()
        self.forward(h, off)

    def finish(self):
        for h in range(2):
            for off in self.p.offs:
                c = self.cross(h, off)
                c.wait_recv()
                c.wait_send()
                for to, dev in self.hops(h, off):
                    self.link(h, off, to, dev).wait_send()


class Reduce:
    def __init__(self, place, part, rc, rb, ssem, rsem):
        self.p, self.part, self.rc, self.rb, self.ssem, self.rsem = place, part, rc, rb, ssem, rsem
        self.half = part.shape[1] // 2

    def rows(self, h):
        return pl.ds(h * self.half, self.half)

    def cross(self, h, off):
        p, k = self.p, self.p.num(off)
        return pltpu.make_async_remote_copy(
            src_ref=self.part.at[p.partner(off), self.rows(h)], dst_ref=self.rc.at[k, self.rows(h)],
            send_sem=self.ssem.at[1, h, k], recv_sem=self.rsem.at[1, h, k],
            device_id=(p.partner(),), device_id_type=MESHID)

    def step_dim(self, h, off):
        return [k for k in reversed(ORDERS[h]) if off[k]][0]

    def link(self, h, off):
        p, k = self.p, self.p.num(off)
        dim = self.step_dim(h, off)
        return pltpu.make_async_remote_copy(
            src_ref=self.part.at[p.dev(off), self.rows(h)], dst_ref=self.rb.at[k, self.rows(h)],
            send_sem=self.ssem.at[0, h, k], recv_sem=self.rsem.at[0, h, k],
            device_id=(p.dev(unit(dim, off[dim])),), device_id_type=MESHID)

    def sources(self, h, off):
        order = ORDERS[h]
        last = max([j for j in range(3) if off[order[j]]], default=-1)
        for j in reversed(range(last + 1, 3)):
            k = order[j]
            for o in range(1, self.p.dims[k]):
                yield tuple(a + b for a, b in zip(off, unit(k, o)))

    def order(self):
        offs = sorted(self.p.offs, key=lambda o: (-sum(1 for a in o if a), o))
        return [(h, o) for o in offs for h in range(2)]

    def begin(self):
        for h, off in self.order():
            self.cross(h, off).start()

    def total(self, h, off):
        p, k = self.p, self.p.num(off)
        self.cross(h, off).wait_recv()
        acc = self.part[p.dev(off), self.rows(h), :].astype(F32) + self.rc[k, self.rows(h), :].astype(F32)
        for s in self.sources(h, off):
            self.link(h, s).wait_recv()
            acc += self.rb[p.num(s), self.rows(h), :].astype(F32)
        return acc

    def advance(self, h, off):
        acc = self.total(h, off)
        if any(off):
            self.part[self.p.dev(off), self.rows(h), :] = acc.astype(BF16)
            self.link(h, off).start()
        return acc

    def finish(self):
        for h, off in self.order():
            self.cross(h, off).wait_send()
            if any(off):
                self.link(h, off).wait_send()


class Sizes:
    def __init__(self, n):
        up = lambda v, m: -(-v // m) * m
        self.n = n
        self.q, self.o, self.f = 3 * D * D // n // 128, D * D // n // 128, D * FF // n // 128
        self.norm, self.bias = 4 * D // n, (4 * D + FF) // n
        self.small = up(self.q, 16)
        self.r0 = up(self.small + 16, 32)
        self.f1 = up(self.o, 16)
        self.f2 = self.f1 + up(self.f, 16)
        self.r1 = up(self.f2 + up(self.f, 16), 32)


def sems(n):
    return [pltpu.SemaphoreType.DMA((2, 2, n // 2))] * 2


def levels(events):
    groups = {}
    for h, off in events:
        groups.setdefault(sum(1 for a in off if a), []).append((h, off))
    return groups


def at_step(i, k):
    return pl.when(i == k)


def unpack(z, buf, first, count, fl, w):
    def one(d, _):
        fl[pl.ds(d * count, count), :] = buf[d, first:first + -(-count // 16) * 16, :].astype(F32)[:count]
        return 0

    lax.fori_loop(0, z.n, one, 0)
    rows, cols = w.shape[0], w.shape[1] // 128
    for j in range(cols):
        w[:, 128 * j:128 * j + 128] = fl[pl.ds(j, rows, stride=cols), :].astype(BF16)


def unpack_small(z, buf, st, sml):
    lane = lax.broadcasted_iota(jnp.int32, (1, 128), 1)

    def put(v, d, size, base):
        shift, first = lax.rem(d * size, 128), d * size // 128
        v = pltpu.roll(v, shift, axis=1)
        sml[pl.ds(base + first, 1), :] += jnp.where(lane >= shift, v, 0.0)
        sml[pl.ds(base + first + 1, 1), :] += jnp.where(lane < shift, v, 0.0)

    def one(d, _):
        st[:16, :] = buf[d, z.small:z.small + 16, :].astype(F32)
        put(st[0:1, :], d, z.norm, 0)
        put(st[1:2, :], d, z.bias, BIAS_ROW)
        return 0

    lax.fori_loop(0, z.n, one, 0)


def flatten(g, fl):
    rows, cols = g.shape[0], g.shape[1] // 128
    for j in range(cols):
        fl[pl.ds(j, rows, stride=cols), :] = g[:, 128 * j:128 * j + 128]


def pack(z, fl, count, first, part):
    size = -(-count // 16) * 16

    def one(d, _):
        part[d, first:first + size, :] = fl[pl.ds(d * count, size), :].astype(BF16)
        return 0

    lax.fori_loop(0, z.n, one, 0)


def pack_small(z, gsm, gqv, gn1, sm, st, part):
    sm[...] = jnp.zeros_like(sm)
    st[...] = jnp.zeros_like(st)

    def put(ref, first, count, base):
        total = jnp.sum(ref[:, first:first + 128 * count], axis=0, keepdims=True)
        for j in range(count):
            sm[base + j:base + j + 1, :] = total[:, 128 * j:128 * j + 128]

    put(gn1, 0, 6, 0)
    put(gsm, 2 * D, 6, 6)
    put(gqv, 0, 6, BIAS_ROW)
    put(gsm, 6 * D, 18, BIAS_ROW + 6)
    lane = lax.broadcasted_iota(jnp.int32, (1, 128), 1)

    def take(d, size, base):
        shift, first = lax.rem(d * size, 128), d * size // 128
        v = jnp.where(lane >= shift, sm[pl.ds(base + first, 1), :], sm[pl.ds(base + first + 1, 1), :])
        return pltpu.roll(v, lax.rem(128 - shift, 128), axis=1)

    def one(d, _):
        st[0:1, :] = take(d, z.norm, 0)
        st[1:2, :] = take(d, z.bias, BIAS_ROW)
        part[d, z.small:z.small + 16, :] = st[:16, :].astype(BF16)
        return 0

    lax.fori_loop(0, z.n, one, 0)


def kernel1(n, s, b, x_ref, q_in, o_in, f1_in, f2_in, n_in, b_in, q_ref, k_ref, v_ref, p_ref, o_ref,
            wqkv, wo, w1, w2, sml, xp, h1, x0, x1, buf0, buf1, fl, st, s0, r0, s1, r1):
    i, last = pl.program_id(0), s.n // b - 1
    z = Sizes(n)
    place = Place(n)
    a, c = Gather(place, x0, buf0, s0, r0), Gather(place, x1, buf1, s1, r1)

    @pl.when(i == 0)
    def _():
        zero(xp, sml, st, x0, x1)
        st[0:1, :z.norm] = n_in[...].astype(F32)
        st[1:2, :z.bias] = b_in[...].astype(F32)
        x0[:z.q, :] = q_in[...]
        x0[z.small:z.small + 16, :] = st[:16, :].astype(BF16)
        x1[:z.o, :] = o_in[...]
        x1[z.f1:z.f1 + z.f, :] = f1_in[...]
        x1[z.f2:z.f2 + z.f, :] = f2_in[...]
        buf0[place.me] = x0[...]
        buf1[place.me] = x1[...]
        greet(place)
        a.begin()
        c.begin()
        for h, off in a.arrivals():
            a.arrive(h, off)
        a.finish()
        unpack_small(z, buf0, st, sml)
        unpack(z, buf0, 0, z.q, fl, wqkv)

    attn_fwd(s, b, x_ref, wqkv, sml, q_ref, k_ref, v_ref, p_ref, o_ref, xp, h1, None, None)

    for level, events in levels(c.arrivals()).items():
        @pl.when(i == min(2 * level, last))
        def _():
            for h, off in events:
                c.arrive(h, off)

    @pl.when(i == last)
    def _():
        c.finish()
        unpack(z, buf1, 0, z.o, fl, wo)
        unpack(z, buf1, z.f1, z.f, fl, w1)
        unpack(z, buf1, z.f2, z.f, fl, w2)


def call1(n, tokens, shards):
    s, z = Pad(tokens), Sizes(n)
    b = s.step(2)
    rows = b * s.rows
    saved = [((s.lanes, D), BF16), ((s.rows, D), BF16), ((s.rows, D), BF16), ((PAIRS, s.rows, 2 * s.lanes), BF16), ((s.rows, D), BF16)]
    whole = [((D, 3 * D), BF16), ((D, D), BF16), ((D, FF), BF16), ((FF, D), BF16), ((48, 128), F32)]
    return pl.pallas_call(
        functools.partial(kernel1, n, s, b), grid=(s.n // b,),
        in_specs=[img(b, s.len, D)] + [const(*v.shape) for v in shards],
        out_specs=[img(b, *v[0]) for v in saved] + [const(*v[0]) for v in whole],
        out_shape=[SDS((s.n,) + v[0], v[1]) for v in saved] + [SDS(*v) for v in whole],
        scratch_shapes=[VM((rows, D), BF16), VM((rows, D), BF16), VM((z.r0, 128), BF16), VM((z.r1, 128), BF16),
                        VM((n, z.r0, 128), BF16), VM((n, z.r1, 128), BF16), VM((4608 + 16, 128), F32), VM((16, 128), F32)] + sems(n) + sems(n),
        compiler_params=big(collective_id=0, has_side_effects=True))(tokens, *shards)


def kernel2(n, s, b, ch, valid, x_ref, c_ref, o_ref, wo, w1, w2, sml, out_ref, gx_ref, go_ref, part, gsm,
            xp, cp, os_, n2s, h2s, as_, gzs, x1s, gout, gfc1, gfc2, fl):
    i = pl.program_id(0)
    z = Sizes(n)

    @pl.when(i == 0)
    def _():
        zero(xp, cp, gout, gfc1, gfc2, gsm)

    ffn(s, b, ch, i, valid, x_ref, c_ref, o_ref, wo, w1, w2, sml,
        out_ref, gx_ref, go_ref, gout, gfc1, gfc2, gsm, xp, cp, os_, n2s, h2s, as_, gzs, x1s)

    @pl.when(i == s.n // b - 1)
    def _():
        zero(part)
        for g, count, first in ((gout, z.o, 0), (gfc1, z.f, z.f1), (gfc2, z.f, z.f2)):
            flatten(g, fl)
            pack(z, fl, count, first, part)


def call2(n, valid, tokens, cot, o, wo, w1, w2, sml):
    s, z = Pad(tokens), Sizes(n)
    b = s.step(3)
    rows = b * s.rows
    grid_spec = pltpu.PrefetchScalarGridSpec(
        num_scalar_prefetch=1, grid=(s.n // b,),
        in_specs=[img(b, s.len, D), img(b, s.len, D), img(b, s.rows, D), const(D, D), const(D, FF), const(FF, D), const(48, 128)],
        out_specs=[img(b, s.len, D), img(b, s.rows, D), img(b, s.lanes, D), const(n, z.r1, 128), const(8, 8 * D + FF)],
        scratch_shapes=[VM((rows, D), BF16), VM((rows, D), BF16), VM((rows, D), BF16), VM((rows, D), F32), VM((rows, D), BF16),
                        VM((rows, FF), BF16), VM((rows, FF), BF16), VM((rows, D), F32),
                        VM((D, D), F32), VM((D, FF), F32), VM((FF, D), F32), VM((4608 + 16, 128), F32)])
    return pl.pallas_call(
        functools.partial(kernel2, n, s, b, 256), grid_spec=grid_spec,
        out_shape=[SDS(tokens.shape, BF16), SDS((s.n, s.rows, D), F32), SDS((s.n, s.lanes, D), BF16),
                   SDS((n, z.r1, 128), BF16), SDS((8, 8 * D + FF), F32)],
        compiler_params=big())(valid, tokens, cot, o, wo, w1, w2, sml)


def kernel3(n, s, b, q_ref, k_ref, v_ref, p_ref, go_ref, part_in, gt_ref, gqv, res, part, rc, rb, s1, r1, local):
    i, last = pl.program_id(0), s.n // b - 1
    place = Place(n)
    r = Reduce(place, part, rc, rb, s1, r1)

    @pl.when(i == 0)
    def _():
        copy = pltpu.make_async_copy(part_in, part, local)
        copy.start()
        zero(gqv)
        greet(place)
        copy.wait()
        r.begin()

    attn_bwd(s, b, q_ref, k_ref, v_ref, p_ref, go_ref, gt_ref, gqv)

    for level, events in levels(r.order()).items():
        @pl.when(i == min(1 + 2 * (3 - level), last))
        def _():
            for h, off in events:
                acc = r.advance(h, off)
                if not any(off):
                    res[r.rows(h), :] = acc

    @pl.when(i == last)
    def _():
        r.finish()


def call3(n, s, q, k, v, p, go, part):
    z = Sizes(n)
    b = s.step(2)
    c = n // 2
    return pl.pallas_call(
        functools.partial(kernel3, n, s, b), grid=(s.n // b,),
        in_specs=[img(b, s.lanes, D), img(b, s.rows, D), img(b, s.rows, D), img(b, PAIRS, s.rows, 2 * s.lanes), img(b, s.lanes, D),
                  pl.BlockSpec(memory_space=pl.ANY)],
        out_specs=[img(b, s.rows, 3 * D), const(8, 2 * D), const(z.r1, 128)],
        out_shape=[SDS((s.n, s.rows, 3 * D), BF16), SDS((8, 2 * D), F32), SDS((z.r1, 128), F32)],
        scratch_shapes=[VM((n, z.r1, 128), BF16), VM((c, z.r1, 128), BF16), VM((c, z.r1, 128), BF16)] + sems(n) + [pltpu.SemaphoreType.DMA],
        compiler_params=big(collective_id=1, has_side_effects=True))(q, k, v, p, go, part)


def kernel4(n, s, b, x_ref, gt_ref, gx_ref, wqkv, sml, gsm, gqv, res, dx_ref, part, oo, o1, o2, gqkv, gn1, xp, h1, gts, fl, sm, st):
    i = pl.program_id(0)
    z = Sizes(n)

    @pl.when(i == 0)
    def _():
        zero(xp, gqkv, gn1)
        oo[...] = res[:z.o, :]
        o1[...] = res[z.f1:z.f1 + z.f, :]
        o2[...] = res[z.f2:z.f2 + z.f, :]

    proj_bwd(s, b, x_ref, gt_ref, gx_ref, wqkv, sml, dx_ref, gqkv, gn1, xp, h1, gts)

    @pl.when(i == s.n // b - 1)
    def _():
        zero(part)
        flatten(gqkv, fl)
        pack(z, fl, z.q, 0, part)
        pack_small(z, gsm, gqv, gn1, sm, st, part)


def call4(n, tokens, gt, gx, wqkv, sml, gsm, gqv, res):
    s, z = Pad(tokens), Sizes(n)
    b = s.step(3)
    rows = b * s.rows
    shards = [(z.o, 128), (z.f, 128), (z.f, 128)]
    return pl.pallas_call(
        functools.partial(kernel4, n, s, b), grid=(s.n // b,),
        in_specs=[img(b, s.len, D), img(b, s.rows, 3 * D), img(b, s.rows, D), const(D, 3 * D), const(48, 128),
                  const(8, 8 * D + FF), const(8, 2 * D), const(z.r1, 128)],
        out_specs=[img(b, s.len, D), const(n, z.r0, 128)] + [const(*v) for v in shards],
        out_shape=[SDS(tokens.shape, F32), SDS((n, z.r0, 128), BF16)] + [SDS(v, F32) for v in shards],
        scratch_shapes=[VM((D, 3 * D), F32), VM((8, 2 * D), F32), VM((rows, D), BF16), VM((rows, D), BF16), VM((rows, 3 * D), BF16),
                        VM((3456 + 16, 128), F32), VM((48, 128), F32), VM((16, 128), F32)],
        compiler_params=big())(tokens, gt, gx, wqkv, sml, gsm, gqv, res)


def kernel5(n, part_in, res, part, rc, rb, s0, r0, local):
    place = Place(n)
    r = Reduce(place, part, rc, rb, s0, r0)
    copy = pltpu.make_async_copy(part_in, part, local)
    copy.start()
    greet(place)
    copy.wait()
    r.begin()
    for h, off in r.order():
        acc = r.advance(h, off)
        if not any(off):
            res[r.rows(h), :] = acc
    r.finish()


def call5(n, part):
    z, c = Sizes(n), n // 2
    return pl.pallas_call(
        functools.partial(kernel5, n), in_specs=[pl.BlockSpec(memory_space=pl.ANY)], out_specs=pl.BlockSpec(memory_space=VM),
        out_shape=SDS((z.r0, 128), F32),
        scratch_shapes=[VM((n, z.r0, 128), BF16), VM((c, z.r0, 128), BF16), VM((c, z.r0, 128), BF16)] + sems(n) + [pltpu.SemaphoreType.DMA],
        compiler_params=big(collective_id=2, has_side_effects=True))(part)


def kernel6(n, res, oq, on, ob):
    z = Sizes(n)
    oq[...] = res[:z.q, :]
    on[...] = res[z.small:z.small + 1, :z.norm]
    ob[...] = res[z.small + 1:z.small + 2, :z.bias]


def call6(n, res):
    z = Sizes(n)
    return pl.pallas_call(functools.partial(kernel6, n), out_shape=[SDS((z.q, 128), F32), SDS((1, z.norm), F32), SDS((1, z.bias), F32)])(res)


def local(n, tokens, cotangent, valid_slots, qkv_weight, out_weight, fc1_weight, fc2_weight, norm_params, bias_params):
    shards = [v.reshape(-1, 128) for v in (qkv_weight, out_weight, fc1_weight, fc2_weight)]
    shards += [norm_params.reshape(1, -1), bias_params.reshape(1, -1)]
    s = Pad(tokens)
    q, k, v, p, o, wqkv, wo, w1, w2, sml = call1(n, tokens, shards)
    out, gx, go, part1, gsm = call2(n, valid_slots, tokens, cotangent, o, wo, w1, w2, sml)
    gt, gqv, res1 = call3(n, s, q, k, v, p, go, part1)
    dx, part0, oo, o1, o2 = call4(n, tokens, gt, gx, wqkv, sml, gsm, gqv, res1)
    oq, on, ob = call6(n, call5(n, part0))
    return (out, dx) + tuple(v.reshape(-1) for v in (oq, oo, o1, o2, on, ob))


def solution(mesh):
    s3, s1 = P("dev", None, None), P("dev")
    return jax.shard_map(functools.partial(local, mesh.shape["dev"]), mesh=mesh, in_specs=(s3, s3) + (s1,) * 7,
                         out_specs=(s3, s3) + (s1,) * 6, check_vma=False)
```

```python
import functools
import jax
import jax.numpy as jnp
from jax import lax
from jax.experimental import pallas as pl
from jax.experimental.pallas import tpu as pltpu
from jax.sharding import PartitionSpec as P

D, HEADS, HEAD_DIM, FF = 384, 6, 64, 1536
PAIRS = HEADS // 2
EPS = 1e-6
F32, BF16 = jnp.float32, jnp.bfloat16
RS2 = 0.7071067811865476
RS2PI = 0.3989422804014327
VM = pltpu.VMEM
BIAS_ROW = 16
SDS = jax.ShapeDtypeStruct


def nn(a, b):
    return lax.dot_general(a, b, (((1,), (0,)), ((), ())), preferred_element_type=F32)


def nt(a, b):
    return lax.dot_general(a, b, (((1,), (1,)), ((), ())), preferred_element_type=F32)


def tn(a, b):
    return lax.dot_general(a, b, (((0,), (0,)), ((), ())), preferred_element_type=F32)


def col8(v):
    return v.reshape(v.shape[0] // 8, 8, v.shape[1]).sum(axis=0)


def norm_fwd(v):
    c = v - jnp.mean(v, axis=1, keepdims=True)
    r = lax.rsqrt(jnp.mean(c * c, axis=1, keepdims=True) + EPS)
    return c * r, r


def norm_bwd(g, n, r, gain):
    e = g * gain
    return r * (e - jnp.mean(e, axis=1, keepdims=True) - n * jnp.mean(e * n, axis=1, keepdims=True))


def vec(sml, row, count=3):
    return jnp.concatenate([sml[row + j:row + j + 1, :] for j in range(count)], axis=1)


def low_lanes():
    return lax.broadcasted_iota(jnp.int32, (1, 128), 1) < 64


def stacked(v):
    low, z = low_lanes(), jnp.zeros_like(v)
    return jnp.concatenate([jnp.where(low, v, z), jnp.where(low, z, v)], axis=0)


class Pad:
    def __init__(self, tokens):
        self.n, self.len, _ = tokens.shape
        self.rows = -(-self.len // 16) * 16
        self.lanes = -(-self.len // 128) * 128

    def step(self, most):
        return max(b for b in range(1, most + 1) if self.n % b == 0)


def staged(items, *stages):
    held = {}
    for tick in range(len(items) + len(stages) - 1):
        for j in range(len(stages)):
            k = tick - j
            if 0 <= k < len(items):
                held[k] = stages[j](items[k], held.get(k))


def attn_fwd(s, b, h1, wqkv, sml, q_ref, k_ref, v_ref, p_ref, o_ref):
    lp, qp, low = s.rows, s.lanes, low_lanes()
    t = nn(h1[...], wqkv[...])
    q = (t[:, :D] + vec(sml, BIAS_ROW)).astype(BF16) * BF16(0.125)
    k = t[:, D:2 * D].astype(BF16)
    v = (t[:, 2 * D:] + vec(sml, BIAS_ROW + 3)).astype(BF16)
    for u in range(b):
        rows = slice(u * lp, u * lp + lp)
        q_ref[u, :lp, :] = q[rows]
        q_ref[u, lp:, :] = jnp.zeros((qp - lp, D), BF16)
        k_ref[u] = k[rows]
        v_ref[u] = v[rows]

    def scores(item, _):
        u, j = item
        cols = slice(128 * j, 128 * j + 128)
        return nt(k_ref[u, :, cols], stacked(q_ref[u, :, cols]))

    def softmax(item, st):
        u, j = item
        cols = slice(128 * j, 128 * j + 128)
        top, bot = st[:lp - 16], st[lp - 16:]
        row = lax.broadcasted_iota(jnp.int32, bot.shape, 0) + (lp - 16)
        bot = jnp.where(row < s.len, bot, -1e30)
        mx = jnp.maximum(jnp.max(top, axis=0, keepdims=True), jnp.max(bot, axis=0, keepdims=True))
        e = jnp.exp(jnp.concatenate([top, bot], axis=0) - mx)
        p = (e * (1.0 / jnp.sum(e, axis=0, keepdims=True))).astype(BF16)
        p_ref[u, j] = p

    def mix(item, _):
        u, j = item
        cols = slice(128 * j, 128 * j + 128)
        p, v = p_ref[u, j], v_ref[u, :, cols]
        o_ref[u, :, cols] = jnp.where(low, tn(p[:, :lp], v), tn(p[:, qp:qp + lp], v)).astype(BF16)

    staged([(u, j) for u in range(b) for j in range(PAIRS)], scores, softmax, mix)


def attn_bwd(s, b, q_ref, k_ref, v_ref, p_ref, go_ref, gt_ref, gts, gcs):
    lp, qp, low = s.rows, s.lanes, low_lanes()

    def first(item, _):
        u, j = item
        cols = slice(128 * j, 128 * j + 128)
        p, go = p_ref[u, j], go_ref[u, :, cols]
        gp = nt(v_ref[u, :, cols], stacked(go))
        gv = jnp.where(low, nn(p[:, :qp], go), nn(p[:, qp:], go))
        return gp, gv

    def middle(item, got):
        u, j = item
        gp, gv = got
        pf = p_ref[u, j].astype(F32)
        return (pf * (gp - jnp.sum(gp * pf, axis=0, keepdims=True))).astype(BF16), gv

    def rest(item, got):
        u, j = item
        gs, gv = got
        cols = slice(128 * j, 128 * j + 128)
        k, q = k_ref[u, :, cols], q_ref[u, :, cols]
        gq = jnp.where(low, tn(gs[:, :lp], k), tn(gs[:, qp:qp + lp], k)) * 0.125
        gk = jnp.where(low, nn(gs[:, :qp], q), nn(gs[:, qp:], q))
        for part, g in enumerate((gq, gk, gv)):
            here = slice(part * D + 128 * j, part * D + 128 * j + 128)
            gcs[:, here] += col8(g)
            g = g.astype(BF16)
            gt_ref[u, :, here] = g
            gts[u * lp:u * lp + lp, here] = g

    staged([(u, j) for u in range(b) for j in range(PAIRS)], first, middle, rest)


LOG2E = 1.4426950408889634
LOG2_2C = 0.17425193526384086
ROOT2 = 1.4142135623730951


def ffn(s, b, sb, ch, i, valid, x_ref, c_ref, o_ref, wo, w1x, w2, w2t, sml,
        out_ref, gx_ref, go_ref, gout, gfc1, gfc2t, gsm, xp, cp, ch_, os_, n2s, r2s, h2s, as_, gzs, x1s, gxb):
    lp, qp = s.rows, s.lanes
    g2, c2 = vec(sml, 6), vec(sml, 9)
    bo, b2 = vec(sml, BIAS_ROW + 6), vec(sml, BIAS_ROW + 21)
    sr = sb * lp
    rows_all = b * lp

    def sub(t, _):
        for u in range(sb):
            w = t * sb + u
            m = valid[i * b + w].astype(BF16)
            xp[u * lp:u * lp + s.len, :] = x_ref[w]
            r0 = pl.multiple_of(w * lp, lp)
            cp[pl.ds(r0, s.len), :] = c_ref[w] * m
            os_[pl.ds(r0, lp), :] = o_ref[w]
        rows = pl.ds(pl.multiple_of(t * sr, sr), sr)
        x1 = xp[...].astype(F32) + nn(os_[rows, :], wo[...]) + bo
        x1s[rows, :] = x1
        n2, r2 = norm_fwd(x1)
        n2s[rows, :] = n2
        r2s[rows, :] = r2
        h2s[rows, :D] = (n2 * g2 + c2).astype(BF16)
        ch_[...] = cp[rows, :] * BF16(0.5)
        for c in range(FF // ch):
            cols = slice(c * ch, (c + 1) * ch)
            z = nn(h2s[rows, :], w1x[:, cols])
            ga = nt(ch_[...], w2[cols, :])
            w = z * RS2
            u1 = 1.0 + lax.erf(w)
            as_[rows, cols] = (w * u1).astype(BF16)
            gzs[rows, cols] = (ga * (u1 + w * jnp.exp2(w * w * -LOG2E + LOG2_2C))).astype(BF16)
        return 0

    lax.fori_loop(0, b // sb, sub, 0)
    yt = nt(w2t[...], as_[...])
    gt = nt(w1x[:D, :], gzs[...])
    y = yt.T[:rows_all] * RS2 + x1s[...] + b2
    for u in range(b):
        out_ref[u] = (y[u * lp:u * lp + s.len] * valid[i * b + u].astype(F32)).astype(BF16)
    gh2 = gt.T[:rows_all]
    n2 = n2s[...]
    gy = cp[:rows_all, :].astype(F32)
    gsm[:, 2 * D:3 * D] += col8(gh2 * n2)
    gsm[:, 3 * D:4 * D] += col8(gh2)
    gsm[:, 7 * D + FF:] += col8(gy)
    gx1 = gy + norm_bwd(gh2, n2, r2s[...], g2)
    gsm[:, 6 * D:7 * D] += col8(gx1)
    gxb[:rows_all, :] = gx1.astype(BF16)
    gfc2t[...] += tn(cp[...], as_[...])
    gfc1[...] += tn(h2s[:, :D + 16], gzs[...])
    gout[...] += tn(os_[...], gxb[...])
    go = nt(gxb[:rows_all, :], wo[...]).astype(BF16)
    for u in range(b):
        gx_ref[u] = gx1[u * lp:u * lp + lp]
        go_ref[u, :lp, :] = go[u * lp:u * lp + lp]
        go_ref[u, lp:, :] = jnp.zeros((qp - lp, D), BF16)


def ffn_setup(s, b, w1, w2, sml, w1x, w2t, h2s):
    w1x[:D, :] = w1[...]
    w1x[D:D + 16, :] = jnp.concatenate([vec(sml, BIAS_ROW + 9, 12), jnp.zeros((15, FF), F32)], axis=0).astype(BF16)
    w1x[D + 16:, :] = jnp.zeros((112, FF), BF16)
    w2t[...] = w2[...].T
    lane = lax.broadcasted_iota(jnp.int32, (b * s.rows, 128), 1)
    h2s[:b * s.rows, D:] = jnp.where(lane == 0, 1.0, 0.0).astype(BF16)


def proj_bwd(s, b, x_ref, gt_ref, gx_ref, wqkv, sml, dx_ref, xp, gts):
    lp = s.rows
    for u in range(b):
        xp[u * lp:u * lp + s.len, :] = x_ref[u]
        gts[u * lp:u * lp + lp, :] = gt_ref[u]
    n1, r1 = norm_fwd(xp[...].astype(F32))
    back = norm_bwd(nt(gts[...], wqkv[...]), n1, r1, vec(sml, 0))
    for u in range(b):
        dx_ref[u] = gx_ref[u, :s.len] + back[u * lp:u * lp + s.len]


def zero(*refs):
    for r in refs:
        r[...] = jnp.zeros_like(r)


def img(b, *shape):
    return pl.BlockSpec((b,) + shape, lambda i, *_: (i,) + (0,) * len(shape))


def const(*shape):
    return pl.BlockSpec(shape, lambda i, *_: (0,) * len(shape), pipeline_mode=pl.Buffered(1))


def big(**kw):
    return pltpu.CompilerParams(vmem_limit_bytes=62 << 20, **kw)


MESHID = pl.DeviceIdType.MESH


def chip_dims(n):
    chips = n // 2
    side = 4 if chips >= 64 else 2
    return (chips // (side * side), side, side)


class Place:
    def __init__(self, n):
        self.n, self.dims = n, chip_dims(n)
        me = lax.axis_index("dev")
        self.me, self.core = me, lax.rem(me, 2)
        s0, s1, s2 = self.dims
        chip = me // 2
        self.at = (chip // (s1 * s2), lax.rem(chip // s2, s1), lax.rem(chip, s2))
        self.offs = [(a, b, c) for a in range(s0) for b in range(s1) for c in range(s2)]

    def chip(self, off):
        i0, i1, i2 = (lax.rem(i + s + o, s) for i, s, o in zip(self.at, self.dims, off))
        return (i0 * self.dims[1] + i1) * self.dims[2] + i2

    def dev(self, off):
        return 2 * self.chip(off) + self.core

    def partner(self, off=(0, 0, 0)):
        return 2 * self.chip(off) + 1 - self.core

    def num(self, off):
        return (off[0] * self.dims[1] + off[1]) * self.dims[2] + off[2]

    def peers(self):
        for k in range(3):
            for o in range(1, self.dims[k]):
                yield self.dev(unit(k, o))
        yield self.partner()


def unit(k, o):
    return tuple(o if j == k else 0 for j in range(3))


def neg(off):
    return tuple(-o for o in off)


def greet(pl_):
    barrier = pltpu.get_barrier_semaphore()
    count = 0
    for dev in pl_.peers():
        pl.semaphore_signal(barrier, inc=1, device_id=(dev,), device_id_type=MESHID)
        count += 1
    pl.semaphore_wait(barrier, count)


ORDERS = ((0, 2, 1), (0, 1, 2))


class Gather:
    def __init__(self, place, src, buf, ssem, rsem):
        self.p, self.src, self.buf, self.ssem, self.rsem = place, src, buf, ssem, rsem
        self.half = src.shape[0] // 2

    def link(self, h, off, to, dev):
        p, rows = self.p, pl.ds(h * self.half, self.half)
        origin = p.dev(neg(off))
        src = self.src.at[rows] if not any(off) else self.buf.at[origin, rows]
        k = p.num(to)
        return pltpu.make_async_remote_copy(
            src_ref=src, dst_ref=self.buf.at[origin, rows], send_sem=self.ssem.at[0, h, k],
            recv_sem=self.rsem.at[0, h, k], device_id=(dev,), device_id_type=MESHID)

    def cross(self, h, off):
        p, rows = self.p, pl.ds(h * self.half, self.half)
        origin = p.dev(neg(off))
        src = self.src.at[rows] if not any(off) else self.buf.at[origin, rows]
        k = p.num(off)
        return pltpu.make_async_remote_copy(
            src_ref=src, dst_ref=self.buf.at[origin, rows], send_sem=self.ssem.at[1, h, k],
            recv_sem=self.rsem.at[1, h, k], device_id=(p.partner(),), device_id_type=MESHID)

    def hops(self, h, off):
        order = ORDERS[h]
        last = max([j for j in range(3) if off[order[j]]], default=-1)
        for j in range(last + 1, 3):
            k = order[j]
            for o in range(1, self.p.dims[k]):
                to = tuple(a + b for a, b in zip(off, unit(k, o)))
                yield to, self.p.dev(unit(k, o))

    def forward(self, h, off):
        for to, dev in self.hops(h, off):
            self.link(h, off, to, dev).start()
        self.cross(h, off).start()

    def begin(self):
        for h in range(2):
            self.forward(h, (0, 0, 0))

    def arrivals(self):
        offs = sorted([o for o in self.p.offs if any(o)], key=lambda o: (sum(1 for a in o if a), min(o[0], self.p.dims[0] - o[0])))
        return [(h, o) for o in offs for h in range(2)]

    def arrive(self, h, off):
        self.link(h, off, off, self.p.me).wait_recv()
        self.forward(h, off)

    def finish(self):
        for h in range(2):
            for off in self.p.offs:
                c = self.cross(h, off)
                c.wait_recv()
                c.wait_send()
                for to, dev in self.hops(h, off):
                    self.link(h, off, to, dev).wait_send()


class Reduce:
    def __init__(self, place, part, rc, rb, ssem, rsem):
        self.p, self.part, self.rc, self.rb, self.ssem, self.rsem = place, part, rc, rb, ssem, rsem
        self.half = part.shape[1] // 2

    def rows(self, h):
        return pl.ds(h * self.half, self.half)

    def cross(self, h, off):
        p, k = self.p, self.p.num(off)
        return pltpu.make_async_remote_copy(
            src_ref=self.part.at[p.partner(off), self.rows(h)], dst_ref=self.rc.at[k, self.rows(h)],
            send_sem=self.ssem.at[1, h, k], recv_sem=self.rsem.at[1, h, k],
            device_id=(p.partner(),), device_id_type=MESHID)

    def step_dim(self, h, off):
        return [k for k in reversed(ORDERS[h]) if off[k]][0]

    def link(self, h, off):
        p, k = self.p, self.p.num(off)
        dim = self.step_dim(h, off)
        return pltpu.make_async_remote_copy(
            src_ref=self.part.at[p.dev(off), self.rows(h)], dst_ref=self.rb.at[k, self.rows(h)],
            send_sem=self.ssem.at[0, h, k], recv_sem=self.rsem.at[0, h, k],
            device_id=(p.dev(unit(dim, off[dim])),), device_id_type=MESHID)

    def sources(self, h, off):
        order = ORDERS[h]
        last = max([j for j in range(3) if off[order[j]]], default=-1)
        for j in reversed(range(last + 1, 3)):
            k = order[j]
            for o in range(1, self.p.dims[k]):
                yield tuple(a + b for a, b in zip(off, unit(k, o)))

    def order(self):
        offs = sorted(self.p.offs, key=lambda o: (-sum(1 for a in o if a), o))
        return [(h, o) for o in offs for h in range(2)]

    def begin(self):
        for h, off in self.order():
            self.cross(h, off).start()

    def total(self, h, off):
        p, k = self.p, self.p.num(off)
        self.cross(h, off).wait_recv()
        acc = self.part[p.dev(off), self.rows(h), :].astype(F32) + self.rc[k, self.rows(h), :].astype(F32)
        for s in self.sources(h, off):
            self.link(h, s).wait_recv()
            acc += self.rb[p.num(s), self.rows(h), :].astype(F32)
        return acc

    def advance(self, h, off):
        acc = self.total(h, off)
        if any(off):
            self.part[self.p.dev(off), self.rows(h), :] = acc.astype(BF16)
            self.link(h, off).start()
        return acc

    def finish(self):
        for h, off in self.order():
            self.cross(h, off).wait_send()
            if any(off):
                self.link(h, off).wait_send()


class Sizes:
    def __init__(self, n):
        up = lambda v, m: -(-v // m) * m
        self.n = n
        self.q, self.o, self.f = 3 * D * D // n // 128, D * D // n // 128, D * FF // n // 128
        self.norm, self.bias = 4 * D // n, (4 * D + FF) // n
        self.small = up(self.q, 16)
        self.r0 = up(self.small + 16, 32)
        self.f1 = up(self.o, 16)
        self.f2 = self.f1 + up(self.f, 16)
        self.r1 = up(self.f2 + up(self.f, 16), 32)


def sems(n):
    return [pltpu.SemaphoreType.DMA((2, 2, n // 2))] * 2


def levels(events):
    groups = {}
    for h, off in events:
        groups.setdefault(sum(1 for a in off if a), []).append((h, off))
    return groups


def at_step(i, k):
    return pl.when(i == k)


def unpack(z, buf, first, count, fl, w):
    def one(d, _):
        fl[pl.ds(d * count, count), :] = buf[d, first:first + -(-count // 16) * 16, :].astype(F32)[:count]
        return 0

    lax.fori_loop(0, z.n, one, 0)
    rows, cols = w.shape[0], w.shape[1] // 128
    for j in range(cols):
        w[:, 128 * j:128 * j + 128] = fl[pl.ds(j, rows, stride=cols), :].astype(BF16)


def unpack_small(z, buf, sml):
    lane = lax.broadcasted_iota(jnp.int32, (1, 128), 1)
    rows = {}

    def put(v, start, size):
        first, shift = divmod(start, 128)
        v = pltpu.roll(v, shift, axis=1) if shift else v
        cut = (lane >= shift) & (lane < shift + size)
        rows[first] = jnp.where(cut, v, rows.get(first, 0.0))
        if shift + size > 128:
            rows[first + 1] = jnp.where(lane < shift + size - 128, v, rows.get(first + 1, 0.0))

    for d in range(z.n):
        v = buf[d, z.small:z.small + 16, :].astype(F32)
        put(v[0:1], d * z.norm, z.norm)
        put(v[1:2], BIAS_ROW * 128 + d * z.bias, z.bias)
    for r, v in rows.items():
        sml[r:r + 1, :] = v


def flatten(g, rows, fl):
    cols = g.shape[1] // 128
    for j in range(cols):
        fl[pl.ds(j, rows, stride=cols), :] = g[:rows, 128 * j:128 * j + 128]


def pack(z, fl, count, first, part):
    size = -(-count // 16) * 16

    def one(d, _):
        part[d, first:first + size, :] = fl[pl.ds(d * count, size), :].astype(BF16)
        return 0

    lax.fori_loop(0, z.n, one, 0)


def column(row):
    return jnp.broadcast_to(row, (128, 128)).T


def finish_qkv(z, nacc, gcs, wqkv, sml, gsm, fl, part):
    total = jnp.sum(gcs[...], axis=0, keepdims=True)
    gain, shift = vec(sml, 0), vec(sml, 3)
    rows = {}
    for a in range(3):
        ra = slice(128 * a, 128 * a + 128)
        g, c = column(gain[:, ra]), column(shift[:, ra])
        q1, q2 = jnp.zeros((128, 128), F32), jnp.zeros((128, 128), F32)
        for j in range(9):
            cols = slice(128 * j, 128 * j + 128)
            na, w = nacc[ra, cols], wqkv[ra, cols].astype(F32)
            fl[pl.ds(9 * 128 * a + j, 128, stride=9), :] = g * na + c * total[:, cols]
            q1 += w * na
            q2 += w * total[:, cols]
        rows[a] = jnp.sum(q1.T, axis=0, keepdims=True)
        rows[3 + a] = jnp.sum(q2.T, axis=0, keepdims=True)
        rows[BIAS_ROW + a] = total[:, 128 * a:128 * a + 128]
        rows[BIAS_ROW + 3 + a] = total[:, 2 * D + 128 * a:2 * D + 128 * a + 128]

    def put(first, count, base):
        v = jnp.sum(gsm[:, first:first + 128 * count], axis=0, keepdims=True)
        for j in range(count):
            rows[base + j] = v[:, 128 * j:128 * j + 128]

    put(2 * D, 6, 6)
    put(6 * D, 18, BIAS_ROW + 6)
    pack(z, fl, z.q, 0, part)
    lane = lax.broadcasted_iota(jnp.int32, (1, 128), 1)

    def take(start, size):
        first, shift = divmod(start, 128)
        v = rows[first]
        if shift + size > 128:
            v = jnp.where(lane >= shift, v, rows[first + 1])
        return pltpu.roll(v, 128 - shift, axis=1) if shift else v

    for d in range(z.n):
        both = [take(d * z.norm, z.norm), take(BIAS_ROW * 128 + d * z.bias, z.bias)]
        part[d, z.small:z.small + 16, :] = jnp.concatenate(both + [jnp.zeros((14, 128), F32)], axis=0).astype(BF16)


def kernel1(n, s, b, x_hbm, q_in, o_in, f1_in, f2_in, n_in, b_in, q_ref, k_ref, v_ref, p_ref, o_ref, n_ref,
            wqkv, wo, w1, w2, sml, tok, n1s, h1, x0, x1, buf0, buf1, fl, st, s0, r0, s1, r1, local):
    i, last = pl.program_id(0), s.n // b - 1
    z = Sizes(n)
    place = Place(n)
    a, c = Gather(place, x0, buf0, s0, r0), Gather(place, x1, buf1, s1, r1)

    def norms(first, past):
        def one(u, _):
            r = pl.multiple_of(u * s.rows, s.rows)
            n1s[pl.ds(r + s.rows - 16, 16), :] = jnp.zeros((16, D), F32)
            n1s[pl.ds(r, s.len), :] = norm_fwd(tok[u].astype(F32))[0]
            return 0

        lax.fori_loop(first, past, one, 0)

    @pl.when(i == 0)
    def _():
        copy = pltpu.make_async_copy(x_hbm, tok, local)
        copy.start()
        zero(sml, st, x0, x1)
        st[0:1, :z.norm] = n_in[...].astype(F32)
        st[1:2, :z.bias] = b_in[...].astype(F32)
        x0[:z.q, :] = q_in[...]
        x0[z.small:z.small + 16, :] = st[:16, :].astype(BF16)
        x1[:z.o, :] = o_in[...]
        x1[z.f1:z.f1 + z.f, :] = f1_in[...]
        x1[z.f2:z.f2 + z.f, :] = f2_in[...]
        buf0[place.me] = x0[...]
        buf1[place.me] = x1[...]
        greet(place)
        a.begin()
        copy.wait()
        groups = levels(a.arrivals())
        for k, level in enumerate(groups):
            norms(k * s.n // len(groups), (k + 1) * s.n // len(groups))
            for h, off in groups[level]:
                a.arrive(h, off)
        a.finish()
        c.begin()
        unpack_small(z, buf0, sml)
        unpack(z, buf0, 0, z.q, fl, wqkv)

    rows = b * s.rows
    n1 = n1s[pl.ds(pl.multiple_of(i * rows, rows), rows), :]
    h1[...] = (n1 * vec(sml, 0) + vec(sml, 3)).astype(BF16)
    for u in range(b):
        n_ref[u] = n1[u * s.rows:(u + 1) * s.rows].astype(BF16)
    attn_fwd(s, b, h1, wqkv, sml, q_ref, k_ref, v_ref, p_ref, o_ref)

    for level, events in levels(c.arrivals()).items():
        @pl.when(i == min(2 * level, last))
        def _():
            for h, off in events:
                c.arrive(h, off)

    @pl.when(i == last)
    def _():
        c.finish()
        unpack(z, buf1, 0, z.o, fl, wo)
        unpack(z, buf1, z.f1, z.f, fl, w1)
        unpack(z, buf1, z.f2, z.f, fl, w2)


def call1(n, tokens, shards):
    s, z = Pad(tokens), Sizes(n)
    b = s.step(2)
    saved = [((s.lanes, D), BF16), ((s.rows, D), BF16), ((s.rows, D), BF16), ((PAIRS, s.rows, 2 * s.lanes), BF16), ((s.rows, D), BF16), ((s.rows, D), BF16)]
    whole = [((D, 3 * D), BF16), ((D, D), BF16), ((D, FF), BF16), ((FF, D), BF16), ((48, 128), F32)]
    return pl.pallas_call(
        functools.partial(kernel1, n, s, b), grid=(s.n // b,),
        in_specs=[pl.BlockSpec(memory_space=pl.ANY)] + [const(*v.shape) for v in shards],
        out_specs=[img(b, *v[0]) for v in saved] + [const(*v[0]) for v in whole],
        out_shape=[SDS((s.n,) + v[0], v[1]) for v in saved] + [SDS(*v) for v in whole],
        scratch_shapes=[VM((s.n, s.len, D), BF16), VM((s.n * s.rows, D), F32), VM((b * s.rows, D), BF16),
                        VM((z.r0, 128), BF16), VM((z.r1, 128), BF16), VM((n, z.r0, 128), BF16), VM((n, z.r1, 128), BF16),
                        VM((4608 + 16, 128), F32), VM((16, 128), F32)] + sems(n) + sems(n) + [pltpu.SemaphoreType.DMA],
        compiler_params=big(collective_id=0, has_side_effects=True))(tokens, *shards)


def kernel2(n, s, b, sb, ch, valid, x_ref, c_ref, o_ref, wo, w1, w2, sml, out_ref, gx_ref, go_ref, part, gsm,
            xp, cp, ch_, os_, n2s, r2s, h2s, as_, gzs, x1s, gxb, w1x, w2t, gout, gfc1, gfc2t, fl):
    i = pl.program_id(0)
    z = Sizes(n)
    rows = b * s.rows

    @pl.when(i == 0)
    def _():
        zero(xp, cp, gout, gfc1, gfc2t, gsm)
        for r in (os_, h2s, as_, gzs, gxb):
            pad = r.shape[0] - rows
            if pad:
                r[rows:, :] = jnp.zeros((pad, r.shape[1]), BF16)
        ffn_setup(s, b, w1, w2, sml, w1x, w2t, h2s)

    ffn(s, b, sb, ch, i, valid, x_ref, c_ref, o_ref, wo, w1x, w2, w2t, sml, out_ref, gx_ref, go_ref,
        gout, gfc1, gfc2t, gsm, xp, cp, ch_, os_, n2s, r2s, h2s, as_, gzs, x1s, gxb)

    @pl.when(i == s.n // b - 1)
    def _():
        zero(part)
        gsm[0:1, 7 * D:7 * D + FF] = gfc1[D:D + 1, :]
        flatten(gout, D, fl)
        pack(z, fl, z.o, 0, part)
        flatten(gfc1, D, fl)
        pack(z, fl, z.f, z.f1, part)
        for j in range(3):
            fl[pl.ds(j, FF, stride=3), :] = gfc2t[128 * j:128 * j + 128, :].T * RS2
        pack(z, fl, z.f, z.f2, part)


def call2(n, valid, tokens, cot, o, wo, w1, w2, sml):
    s, z = Pad(tokens), Sizes(n)
    b = s.step(6)
    sb = max(k for k in range(1, 4) if b % k == 0)
    rows = b * s.rows
    up, sr = -(-rows // 256) * 256, sb * s.rows
    grid_spec = pltpu.PrefetchScalarGridSpec(
        num_scalar_prefetch=1, grid=(s.n // b,),
        in_specs=[img(b, s.len, D), img(b, s.len, D), img(b, s.rows, D), const(D, D), const(D, FF), const(FF, D), const(48, 128)],
        out_specs=[img(b, s.len, D), img(b, s.rows, D), img(b, s.lanes, D), const(n, z.r1, 128), const(8, 8 * D + FF)],
        scratch_shapes=[VM((sr, D), BF16), VM((up, D), BF16), VM((sr, D), BF16), VM((up, D), BF16), VM((rows, D), F32), VM((rows, 1), F32),
                        VM((up, D + 128), BF16), VM((up, FF), BF16), VM((up, FF), BF16), VM((rows, D), F32), VM((up, D), BF16),
                        VM((D + 128, FF), BF16), VM((D, FF), BF16), VM((D, D), F32), VM((D + 16, FF), F32), VM((D, FF), F32),
                        VM((4608 + 16, 128), F32)])
    return pl.pallas_call(
        functools.partial(kernel2, n, s, b, sb, 256), grid_spec=grid_spec,
        out_shape=[SDS(tokens.shape, BF16), SDS((s.n, s.rows, D), F32), SDS((s.n, s.lanes, D), BF16),
                   SDS((n, z.r1, 128), BF16), SDS((8, 8 * D + FF), F32)],
        compiler_params=big())(valid, tokens, cot, o, wo, w1, w2, sml)


def kernel3(n, s, b, q_ref, k_ref, v_ref, p_ref, go_ref, n_ref, wqkv, sml, gsm, part_in, gt_ref, part0, res,
            part, rc, rb, nacc, gcs, n1b, gts, fl, s1, r1, local):
    i, last = pl.program_id(0), s.n // b - 1
    z = Sizes(n)
    place = Place(n)
    r = Reduce(place, part, rc, rb, s1, r1)

    @pl.when(i == 0)
    def _():
        copy = pltpu.make_async_copy(part_in, part, local)
        copy.start()
        zero(nacc, gcs)
        greet(place)
        copy.wait()
        r.begin()

    attn_bwd(s, b, q_ref, k_ref, v_ref, p_ref, go_ref, gt_ref, gts, gcs)
    for u in range(b):
        n1b[u * s.rows:(u + 1) * s.rows, :] = n_ref[u]
    nacc[...] += tn(n1b[...], gts[...])

    @pl.when(i == last)
    def _():
        zero(part0)
        finish_qkv(z, nacc, gcs, wqkv, sml, gsm, fl, part0)

    for level, events in levels(r.order()).items():
        @pl.when(i == min(2 + 2 * (3 - level), last))
        def _():
            for h, off in events:
                acc = r.advance(h, off)
                if not any(off):
                    res[r.rows(h), :] = acc

    @pl.when(i == last)
    def _():
        r.finish()


def call3(n, s, q, k, v, p, go, n1, wqkv, sml, gsm, part):
    z = Sizes(n)
    b = s.step(2)
    c, rows = n // 2, b * s.rows
    return pl.pallas_call(
        functools.partial(kernel3, n, s, b), grid=(s.n // b,),
        in_specs=[img(b, s.lanes, D), img(b, s.rows, D), img(b, s.rows, D), img(b, PAIRS, s.rows, 2 * s.lanes), img(b, s.lanes, D),
                  img(b, s.rows, D), const(D, 3 * D), const(48, 128), const(8, 8 * D + FF), pl.BlockSpec(memory_space=pl.ANY)],
        out_specs=[img(b, s.rows, 3 * D), const(n, z.r0, 128), const(z.r1, 128)],
        out_shape=[SDS((s.n, s.rows, 3 * D), BF16), SDS((n, z.r0, 128), BF16), SDS((z.r1, 128), F32)],
        scratch_shapes=[VM((n, z.r1, 128), BF16), VM((c, z.r1, 128), BF16), VM((c, z.r1, 128), BF16),
                        VM((D, 3 * D), F32), VM((8, 3 * D), F32), VM((rows, D), BF16), VM((rows, 3 * D), BF16),
                        VM((3456 + 16, 128), F32)] + sems(n) + [pltpu.SemaphoreType.DMA],
        compiler_params=big(collective_id=1, has_side_effects=True))(q, k, v, p, go, n1, wqkv, sml, gsm, part)


def kernel4(n, s, b, x_ref, gt_ref, gx_ref, wqkv, sml, part_in, dx_ref, res, part, rc, rb, xp, gts, s0, r0, local):
    i, last = pl.program_id(0), s.n // b - 1
    place = Place(n)
    r = Reduce(place, part, rc, rb, s0, r0)

    @pl.when(i == 0)
    def _():
        copy = pltpu.make_async_copy(part_in, part, local)
        copy.start()
        zero(xp)
        greet(place)
        copy.wait()
        r.begin()

    proj_bwd(s, b, x_ref, gt_ref, gx_ref, wqkv, sml, dx_ref, xp, gts)

    for level, events in levels(r.order()).items():
        @pl.when(i == min(1 + 2 * (3 - level), last))
        def _():
            for h, off in events:
                acc = r.advance(h, off)
                if not any(off):
                    res[r.rows(h), :] = acc

    @pl.when(i == last)
    def _():
        r.finish()


def call4(n, tokens, gt, gx, wqkv, sml, part):
    s, z = Pad(tokens), Sizes(n)
    b = s.step(2)
    c, rows = n // 2, b * s.rows
    return pl.pallas_call(
        functools.partial(kernel4, n, s, b), grid=(s.n // b,),
        in_specs=[img(b, s.len, D), img(b, s.rows, 3 * D), img(b, s.rows, D), const(D, 3 * D), const(48, 128), pl.BlockSpec(memory_space=pl.ANY)],
        out_specs=[img(b, s.len, D), const(z.r0, 128)],
        out_shape=[SDS(tokens.shape, F32), SDS((z.r0, 128), F32)],
        scratch_shapes=[VM((n, z.r0, 128), BF16), VM((c, z.r0, 128), BF16), VM((c, z.r0, 128), BF16),
                        VM((rows, D), BF16), VM((rows, 3 * D), BF16)] + sems(n) + [pltpu.SemaphoreType.DMA],
        compiler_params=big(collective_id=2, has_side_effects=True))(tokens, gt, gx, wqkv, sml, part)


def kernel5(n, dx_in, res0, res1, dx, oq, oo, o1, o2, on, ob):
    z = Sizes(n)
    dx[...] = dx_in[...]

    @pl.when(pl.program_id(0) == 0)
    def _():
        oq[...] = res0[:z.q, :]
        on[...] = res0[z.small:z.small + 1, :z.norm]
        ob[...] = res0[z.small + 1:z.small + 2, :z.bias]
        oo[...] = res1[:z.o, :]
        o1[...] = res1[z.f1:z.f1 + z.f, :]
        o2[...] = res1[z.f2:z.f2 + z.f, :]


def call5(n, dx, res0, res1):
    s, z = Pad(dx), Sizes(n)
    b = s.step(3)
    shapes = [(z.q, 128), (z.o, 128), (z.f, 128), (z.f, 128), (1, z.norm), (1, z.bias)]
    return pl.pallas_call(
        functools.partial(kernel5, n), grid=(s.n // b,),
        in_specs=[img(b, s.len, D), const(z.r0, 128), const(z.r1, 128)],
        out_specs=[img(b, s.len, D)] + [const(*v) for v in shapes],
        out_shape=[SDS(dx.shape, F32)] + [SDS(v, F32) for v in shapes],
        compiler_params=big())(dx, res0, res1)


def local(n, tokens, cotangent, valid_slots, qkv_weight, out_weight, fc1_weight, fc2_weight, norm_params, bias_params):
    shards = [v.reshape(-1, 128) for v in (qkv_weight, out_weight, fc1_weight, fc2_weight)]
    shards += [norm_params.reshape(1, -1), bias_params.reshape(1, -1)]
    s = Pad(tokens)
    q, k, v, p, o, n1, wqkv, wo, w1, w2, sml = call1(n, tokens, shards)
    out, gx, go, part1, gsm = call2(n, valid_slots, tokens, cotangent, o, wo, w1, w2, sml)
    gt, part0, res1 = call3(n, s, q, k, v, p, go, n1, wqkv, sml, gsm, part1)
    dx, res0 = call4(n, tokens, gt, gx, wqkv, sml, part0)
    dx, *grads = call5(n, dx, res0, res1)
    return (out, dx) + tuple(v.reshape(-1) for v in grads)


def solution(mesh):
    s3, s1 = P("dev", None, None), P("dev")
    return jax.shard_map(functools.partial(local, mesh.shape["dev"]), mesh=mesh, in_specs=(s3, s3) + (s1,) * 7,
                         out_specs=(s3, s3) + (s1,) * 6, check_vma=False)
```

```python
import functools
import jax
import jax.numpy as jnp
from jax import lax
from jax.experimental import pallas as pl
from jax.experimental.pallas import tpu as pltpu
from jax.sharding import PartitionSpec as P

D, HEADS, HEAD_DIM, FF = 384, 6, 64, 1536
PAIRS = HEADS // 2
EPS = 1e-6
F32, BF16 = jnp.float32, jnp.bfloat16
RS2 = 0.7071067811865476
RS2PI = 0.3989422804014327
VM = pltpu.VMEM
BIAS_ROW = 16
SDS = jax.ShapeDtypeStruct


def nn(a, b):
    return lax.dot_general(a, b, (((1,), (0,)), ((), ())), preferred_element_type=F32)


def nt(a, b):
    return lax.dot_general(a, b, (((1,), (1,)), ((), ())), preferred_element_type=F32)


def tn(a, b):
    return lax.dot_general(a, b, (((0,), (0,)), ((), ())), preferred_element_type=F32)


def col8(v):
    return v.reshape(v.shape[0] // 8, 8, v.shape[1]).sum(axis=0)


def norm_fwd(v):
    c = v - jnp.mean(v, axis=1, keepdims=True)
    r = lax.rsqrt(jnp.mean(c * c, axis=1, keepdims=True) + EPS)
    return c * r, r


def norm_bwd(g, n, r, gain):
    e = g * gain
    return r * (e - jnp.mean(e, axis=1, keepdims=True) - n * jnp.mean(e * n, axis=1, keepdims=True))


def vec(sml, row, count=3):
    return jnp.concatenate([sml[row + j:row + j + 1, :] for j in range(count)], axis=1)


def low_lanes():
    return lax.broadcasted_iota(jnp.int32, (1, 128), 1) < 64


def stacked(v):
    low, z = low_lanes(), jnp.zeros_like(v)
    return jnp.concatenate([jnp.where(low, v, z), jnp.where(low, z, v)], axis=0)


class Pad:
    def __init__(self, tokens):
        self.n, self.len, _ = tokens.shape
        self.rows = -(-self.len // 16) * 16
        self.lanes = -(-self.len // 128) * 128

    def step(self, most):
        return max(b for b in range(1, most + 1) if self.n % b == 0)


def staged(items, *stages):
    held = {}
    for tick in range(len(items) + len(stages) - 1):
        for j in range(len(stages)):
            k = tick - j
            if 0 <= k < len(items):
                held[k] = stages[j](items[k], held.get(k))


def attn_fwd(s, b, h1, wqkv, sml, q_ref, k_ref, v_ref, p_ref, o_ref):
    lp, qp, low = s.rows, s.lanes, low_lanes()
    t = nn(h1[...], wqkv[...])
    q = (t[:, :D] + vec(sml, BIAS_ROW)).astype(BF16) * BF16(0.125)
    k = t[:, D:2 * D].astype(BF16)
    v = (t[:, 2 * D:] + vec(sml, BIAS_ROW + 3)).astype(BF16)
    for u in range(b):
        rows = slice(u * lp, u * lp + lp)
        q_ref[u, :lp, :] = q[rows]
        q_ref[u, lp:, :] = jnp.zeros((qp - lp, D), BF16)
        k_ref[u] = k[rows]
        v_ref[u] = v[rows]

    def scores(item, _):
        u, j = item
        cols = slice(128 * j, 128 * j + 128)
        return nt(k_ref[u, :, cols], stacked(q_ref[u, :, cols]))

    def softmax(item, st):
        u, j = item
        cols = slice(128 * j, 128 * j + 128)
        top, bot = st[:lp - 16], st[lp - 16:]
        row = lax.broadcasted_iota(jnp.int32, bot.shape, 0) + (lp - 16)
        bot = jnp.where(row < s.len, bot, -1e30)
        mx = jnp.maximum(jnp.max(top, axis=0, keepdims=True), jnp.max(bot, axis=0, keepdims=True))
        e = jnp.exp(jnp.concatenate([top, bot], axis=0) - mx)
        p = (e * (1.0 / jnp.sum(e, axis=0, keepdims=True))).astype(BF16)
        p_ref[u, j] = p

    def mix(item, _):
        u, j = item
        cols = slice(128 * j, 128 * j + 128)
        p, v = p_ref[u, j], v_ref[u, :, cols]
        o_ref[u, :, cols] = jnp.where(low, tn(p[:, :lp], v), tn(p[:, qp:qp + lp], v)).astype(BF16)

    staged([(u, j) for u in range(b) for j in range(PAIRS)], scores, softmax, mix)


def attn_bwd(s, b, q_ref, k_ref, v_ref, p_ref, go_ref, gt_ref, gts, gcs):
    lp, qp, low = s.rows, s.lanes, low_lanes()

    def first(item, _):
        u, j = item
        cols = slice(128 * j, 128 * j + 128)
        p, go = p_ref[u, j], go_ref[u, :, cols]
        gp = nt(v_ref[u, :, cols], stacked(go))
        gv = jnp.where(low, nn(p[:, :qp], go), nn(p[:, qp:], go))
        return gp, gv

    def middle(item, got):
        u, j = item
        gp, gv = got
        pf = p_ref[u, j].astype(F32)
        return (pf * (gp - jnp.sum(gp * pf, axis=0, keepdims=True))).astype(BF16), gv

    def rest(item, got):
        u, j = item
        gs, gv = got
        cols = slice(128 * j, 128 * j + 128)
        k, q = k_ref[u, :, cols], q_ref[u, :, cols]
        gq = jnp.where(low, tn(gs[:, :lp], k), tn(gs[:, qp:qp + lp], k)) * 0.125
        gk = jnp.where(low, nn(gs[:, :qp], q), nn(gs[:, qp:], q))
        for part, g in enumerate((gq, gk, gv)):
            here = slice(part * D + 128 * j, part * D + 128 * j + 128)
            gcs[:, here] += col8(g)
            g = g.astype(BF16)
            gt_ref[u, :, here] = g
            gts[u * lp:u * lp + lp, here] = g

    staged([(u, j) for u in range(b) for j in range(PAIRS)], first, middle, rest)


LOG2E = 1.4426950408889634
LOG2_2C = 0.17425193526384086
ROOT2 = 1.4142135623730951


def ffn(s, b, sb, ch, i, valid, x_ref, c_ref, o_ref, wo, w1x, w2, w2t, sml,
        out_ref, gx_ref, go_ref, gout, gfc1, gfc2t, gsm, xp, cp, ch_, os_, n2s, r2s, h2s, as_, gzs, x1s, gxb):
    lp, qp = s.rows, s.lanes
    g2, c2 = vec(sml, 6), vec(sml, 9)
    bo, b2 = vec(sml, BIAS_ROW + 6), vec(sml, BIAS_ROW + 21)
    sr = sb * lp
    rows_all = b * lp

    def sub(t, _):
        for u in range(sb):
            w = t * sb + u
            m = valid[i * b + w].astype(BF16)
            xp[u * lp:u * lp + s.len, :] = x_ref[w]
            r0 = pl.multiple_of(w * lp, lp)
            cp[pl.ds(r0, s.len), :] = c_ref[w] * m
            os_[pl.ds(r0, lp), :] = o_ref[w]
        rows = pl.ds(pl.multiple_of(t * sr, sr), sr)
        x1 = xp[...].astype(F32) + nn(os_[rows, :], wo[...]) + bo
        x1s[rows, :] = x1
        n2, r2 = norm_fwd(x1)
        n2s[rows, :] = n2
        r2s[rows, :] = r2
        h2s[rows, :D] = (n2 * g2 + c2).astype(BF16)
        ch_[...] = cp[rows, :] * BF16(0.5)
        for c in range(FF // ch):
            cols = slice(c * ch, (c + 1) * ch)
            z = nn(h2s[rows, :], w1x[:, cols])
            ga = nt(ch_[...], w2[cols, :])
            w = z * RS2
            u1 = 1.0 + lax.erf(w)
            as_[rows, cols] = (w * u1).astype(BF16)
            gzs[rows, cols] = (ga * (u1 + w * jnp.exp2(w * w * -LOG2E + LOG2_2C))).astype(BF16)
        return 0

    lax.fori_loop(0, b // sb, sub, 0)
    yt = nt(w2t[...], as_[...])
    gt = nt(w1x[:D, :], gzs[...])
    y = yt.T[:rows_all] * RS2 + x1s[...] + b2
    for u in range(b):
        out_ref[u] = (y[u * lp:u * lp + s.len] * valid[i * b + u].astype(F32)).astype(BF16)
    gh2 = gt.T[:rows_all]
    n2 = n2s[...]
    gy = cp[:rows_all, :].astype(F32)
    gsm[:, 2 * D:3 * D] += col8(gh2 * n2)
    gsm[:, 3 * D:4 * D] += col8(gh2)
    gsm[:, 7 * D + FF:] += col8(gy)
    gx1 = gy + norm_bwd(gh2, n2, r2s[...], g2)
    gsm[:, 6 * D:7 * D] += col8(gx1)
    gxb[:rows_all, :] = gx1.astype(BF16)
    gfc2t[...] += tn(cp[...], as_[...])
    gfc1[...] += tn(h2s[:, :D + 16], gzs[...])
    gout[...] += tn(os_[...], gxb[...])
    go = nt(gxb[:rows_all, :], wo[...]).astype(BF16)
    for u in range(b):
        gx_ref[u] = gxb[u * lp:u * lp + lp, :]
        go_ref[u, :lp, :] = go[u * lp:u * lp + lp]
        go_ref[u, lp:, :] = jnp.zeros((qp - lp, D), BF16)


def ffn_setup(s, b, w1, w2, sml, w1x, w2t, h2s):
    w1x[:D, :] = w1[...]
    w1x[D:D + 16, :] = jnp.concatenate([vec(sml, BIAS_ROW + 9, 12), jnp.zeros((15, FF), F32)], axis=0).astype(BF16)
    w1x[D + 16:, :] = jnp.zeros((112, FF), BF16)
    w2t[...] = w2[...].T
    lane = lax.broadcasted_iota(jnp.int32, (b * s.rows, 128), 1)
    h2s[:b * s.rows, D:] = jnp.where(lane == 0, 1.0, 0.0).astype(BF16)


def proj_bwd(s, b, x_ref, gt_ref, gx_ref, wqkv, sml, dx_ref, xp, gts):
    lp = s.rows
    for u in range(b):
        xp[u * lp:u * lp + s.len, :] = x_ref[u]
        gts[u * lp:u * lp + lp, :] = gt_ref[u]
    n1, r1 = norm_fwd(xp[...].astype(F32))
    back = norm_bwd(nt(gts[...], wqkv[...]), n1, r1, vec(sml, 0))
    for u in range(b):
        dx_ref[u] = (gx_ref[u].astype(F32) + back[u * lp:u * lp + lp]).astype(BF16)[:s.len]


def zero(*refs):
    for r in refs:
        r[...] = jnp.zeros_like(r)


def img(b, *shape):
    return pl.BlockSpec((b,) + shape, lambda i, *_: (i,) + (0,) * len(shape))


def const(*shape):
    return pl.BlockSpec(shape, lambda i, *_: (0,) * len(shape), pipeline_mode=pl.Buffered(1))


def big(**kw):
    return pltpu.CompilerParams(vmem_limit_bytes=62 << 20, **kw)


MESHID = pl.DeviceIdType.MESH


def chip_dims(n):
    chips = n // 2
    side = 4 if chips >= 64 else 2
    return (chips // (side * side), side, side)


class Place:
    def __init__(self, n):
        self.n, self.dims = n, chip_dims(n)
        me = lax.axis_index("dev")
        self.me, self.core = me, lax.rem(me, 2)
        s0, s1, s2 = self.dims
        chip = me // 2
        self.at = (chip // (s1 * s2), lax.rem(chip // s2, s1), lax.rem(chip, s2))
        self.offs = [(a, b, c) for a in range(s0) for b in range(s1) for c in range(s2)]

    def chip(self, off):
        i0, i1, i2 = (lax.rem(i + s + o, s) for i, s, o in zip(self.at, self.dims, off))
        return (i0 * self.dims[1] + i1) * self.dims[2] + i2

    def dev(self, off):
        return 2 * self.chip(off) + self.core

    def partner(self, off=(0, 0, 0)):
        return 2 * self.chip(off) + 1 - self.core

    def num(self, off):
        return (off[0] * self.dims[1] + off[1]) * self.dims[2] + off[2]

    def peers(self):
        for k in range(3):
            for o in range(1, self.dims[k]):
                yield self.dev(unit(k, o))
        yield self.partner()


def unit(k, o):
    return tuple(o if j == k else 0 for j in range(3))


def neg(off):
    return tuple(-o for o in off)


def greet(pl_):
    barrier = pltpu.get_barrier_semaphore()
    count = 0
    for dev in pl_.peers():
        pl.semaphore_signal(barrier, inc=1, device_id=(dev,), device_id_type=MESHID)
        count += 1
    pl.semaphore_wait(barrier, count)


ORDERS = ((0, 2, 1), (0, 1, 2))


class Gather:
    def __init__(self, place, src, buf, ssem, rsem):
        self.p, self.src, self.buf, self.ssem, self.rsem = place, src, buf, ssem, rsem
        self.half = src.shape[0] // 2

    def link(self, h, off, to, dev):
        p, rows = self.p, pl.ds(h * self.half, self.half)
        origin = p.dev(neg(off))
        src = self.src.at[rows] if not any(off) else self.buf.at[origin, rows]
        k = p.num(to)
        return pltpu.make_async_remote_copy(
            src_ref=src, dst_ref=self.buf.at[origin, rows], send_sem=self.ssem.at[0, h, k],
            recv_sem=self.rsem.at[0, h, k], device_id=(dev,), device_id_type=MESHID)

    def cross(self, h, off):
        p, rows = self.p, pl.ds(h * self.half, self.half)
        origin = p.dev(neg(off))
        src = self.src.at[rows] if not any(off) else self.buf.at[origin, rows]
        k = p.num(off)
        return pltpu.make_async_remote_copy(
            src_ref=src, dst_ref=self.buf.at[origin, rows], send_sem=self.ssem.at[1, h, k],
            recv_sem=self.rsem.at[1, h, k], device_id=(p.partner(),), device_id_type=MESHID)

    def hops(self, h, off):
        order = ORDERS[h]
        last = max([j for j in range(3) if off[order[j]]], default=-1)
        for j in range(last + 1, 3):
            k = order[j]
            for o in range(1, self.p.dims[k]):
                to = tuple(a + b for a, b in zip(off, unit(k, o)))
                yield to, self.p.dev(unit(k, o))

    def forward(self, h, off):
        for to, dev in self.hops(h, off):
            self.link(h, off, to, dev).start()
        self.cross(h, off).start()

    def begin(self):
        for h in range(2):
            self.forward(h, (0, 0, 0))

    def arrivals(self):
        offs = sorted([o for o in self.p.offs if any(o)], key=lambda o: (sum(1 for a in o if a), min(o[0], self.p.dims[0] - o[0])))
        return [(h, o) for o in offs for h in range(2)]

    def arrive(self, h, off):
        self.link(h, off, off, self.p.me).wait_recv()
        self.forward(h, off)

    def finish(self):
        for h in range(2):
            for off in self.p.offs:
                c = self.cross(h, off)
                c.wait_recv()
                c.wait_send()
                for to, dev in self.hops(h, off):
                    self.link(h, off, to, dev).wait_send()


class Reduce:
    def __init__(self, place, part, rc, rb, ssem, rsem):
        self.p, self.part, self.rc, self.rb, self.ssem, self.rsem = place, part, rc, rb, ssem, rsem
        self.half = part.shape[1] // 2

    def rows(self, h):
        return pl.ds(h * self.half, self.half)

    def cross(self, h, off):
        p, k = self.p, self.p.num(off)
        return pltpu.make_async_remote_copy(
            src_ref=self.part.at[p.partner(off), self.rows(h)], dst_ref=self.rc.at[k, self.rows(h)],
            send_sem=self.ssem.at[1, h, k], recv_sem=self.rsem.at[1, h, k],
            device_id=(p.partner(),), device_id_type=MESHID)

    def step_dim(self, h, off):
        return [k for k in reversed(ORDERS[h]) if off[k]][0]

    def link(self, h, off):
        p, k = self.p, self.p.num(off)
        dim = self.step_dim(h, off)
        return pltpu.make_async_remote_copy(
            src_ref=self.part.at[p.dev(off), self.rows(h)], dst_ref=self.rb.at[k, self.rows(h)],
            send_sem=self.ssem.at[0, h, k], recv_sem=self.rsem.at[0, h, k],
            device_id=(p.dev(unit(dim, off[dim])),), device_id_type=MESHID)

    def sources(self, h, off):
        order = ORDERS[h]
        last = max([j for j in range(3) if off[order[j]]], default=-1)
        for j in reversed(range(last + 1, 3)):
            k = order[j]
            for o in range(1, self.p.dims[k]):
                yield tuple(a + b for a, b in zip(off, unit(k, o)))

    def order(self):
        offs = sorted(self.p.offs, key=lambda o: (-sum(1 for a in o if a), o))
        return [(h, o) for o in offs for h in range(2)]

    def begin(self):
        for h, off in self.order():
            self.cross(h, off).start()

    def total(self, h, off):
        p, k = self.p, self.p.num(off)
        self.cross(h, off).wait_recv()
        acc = self.part[p.dev(off), self.rows(h), :].astype(F32) + self.rc[k, self.rows(h), :].astype(F32)
        for s in self.sources(h, off):
            self.link(h, s).wait_recv()
            acc += self.rb[p.num(s), self.rows(h), :].astype(F32)
        return acc

    def advance(self, h, off):
        acc = self.total(h, off)
        if any(off):
            self.part[self.p.dev(off), self.rows(h), :] = acc.astype(BF16)
            self.link(h, off).start()
        return acc

    def finish(self):
        for h, off in self.order():
            self.cross(h, off).wait_send()
            if any(off):
                self.link(h, off).wait_send()


class Sizes:
    def __init__(self, n):
        up = lambda v, m: -(-v // m) * m
        self.n = n
        self.q, self.o, self.f = 3 * D * D // n // 128, D * D // n // 128, D * FF // n // 128
        self.norm, self.bias = 4 * D // n, (4 * D + FF) // n
        self.small = up(self.q, 16)
        self.r0 = up(self.small + 16, 32)
        self.f1 = up(self.o, 16)
        self.f2 = self.f1 + up(self.f, 16)
        self.r1 = up(self.f2 + up(self.f, 16), 32)


def sems(n):
    return [pltpu.SemaphoreType.DMA((2, 2, n // 2))] * 2


def levels(events):
    groups = {}
    for h, off in events:
        groups.setdefault(sum(1 for a in off if a), []).append((h, off))
    return groups


def at_step(i, k):
    return pl.when(i == k)


def unpack(z, buf, first, count, fl, w):
    def one(d, _):
        fl[pl.ds(d * count, count), :] = buf[d, first:first + -(-count // 16) * 16, :].astype(F32)[:count]
        return 0

    lax.fori_loop(0, z.n, one, 0)
    rows, cols = w.shape[0], w.shape[1] // 128
    for j in range(cols):
        w[:, 128 * j:128 * j + 128] = fl[pl.ds(j, rows, stride=cols), :].astype(BF16)


def unpack_small(z, buf, sml):
    lane = lax.broadcasted_iota(jnp.int32, (1, 128), 1)
    rows = {}

    def put(v, start, size):
        first, shift = divmod(start, 128)
        v = pltpu.roll(v, shift, axis=1) if shift else v
        cut = (lane >= shift) & (lane < shift + size)
        rows[first] = jnp.where(cut, v, rows.get(first, 0.0))
        if shift + size > 128:
            rows[first + 1] = jnp.where(lane < shift + size - 128, v, rows.get(first + 1, 0.0))

    for d in range(z.n):
        v = buf[d, z.small:z.small + 16, :].astype(F32)
        put(v[0:1], d * z.norm, z.norm)
        put(v[1:2], BIAS_ROW * 128 + d * z.bias, z.bias)
    for r, v in rows.items():
        sml[r:r + 1, :] = v


def flatten(g, rows, fl):
    cols = g.shape[1] // 128
    for j in range(cols):
        fl[pl.ds(j, rows, stride=cols), :] = g[:rows, 128 * j:128 * j + 128]


def pack(z, fl, count, first, part):
    size = -(-count // 16) * 16

    def one(d, _):
        part[d, first:first + size, :] = fl[pl.ds(d * count, size), :].astype(BF16)
        return 0

    lax.fori_loop(0, z.n, one, 0)


def column(row):
    return jnp.broadcast_to(row, (128, 128)).T


def finish_qkv(z, nacc, gcs, wqkv, sml, gsm, fl, part):
    total = jnp.sum(gcs[...], axis=0, keepdims=True)
    gain, shift = vec(sml, 0), vec(sml, 3)
    rows = {}
    for a in range(3):
        ra = slice(128 * a, 128 * a + 128)
        g, c = column(gain[:, ra]), column(shift[:, ra])
        q1, q2 = jnp.zeros((128, 128), F32), jnp.zeros((128, 128), F32)
        for j in range(9):
            cols = slice(128 * j, 128 * j + 128)
            na, w = nacc[ra, cols], wqkv[ra, cols].astype(F32)
            fl[pl.ds(9 * 128 * a + j, 128, stride=9), :] = g * na + c * total[:, cols]
            q1 += w * na
            q2 += w * total[:, cols]
        rows[a] = jnp.sum(q1.T, axis=0, keepdims=True)
        rows[3 + a] = jnp.sum(q2.T, axis=0, keepdims=True)
        rows[BIAS_ROW + a] = total[:, 128 * a:128 * a + 128]
        rows[BIAS_ROW + 3 + a] = total[:, 2 * D + 128 * a:2 * D + 128 * a + 128]

    def put(first, count, base):
        v = jnp.sum(gsm[:, first:first + 128 * count], axis=0, keepdims=True)
        for j in range(count):
            rows[base + j] = v[:, 128 * j:128 * j + 128]

    put(2 * D, 6, 6)
    put(6 * D, 18, BIAS_ROW + 6)
    pack(z, fl, z.q, 0, part)
    lane = lax.broadcasted_iota(jnp.int32, (1, 128), 1)

    def take(start, size):
        first, shift = divmod(start, 128)
        v = rows[first]
        if shift + size > 128:
            v = jnp.where(lane >= shift, v, rows[first + 1])
        return pltpu.roll(v, 128 - shift, axis=1) if shift else v

    for d in range(z.n):
        both = [take(d * z.norm, z.norm), take(BIAS_ROW * 128 + d * z.bias, z.bias)]
        part[d, z.small:z.small + 16, :] = jnp.concatenate(both + [jnp.zeros((14, 128), F32)], axis=0).astype(BF16)


def kernel1(n, s, b, x_hbm, q_in, o_in, f1_in, f2_in, n_in, b_in, q_ref, k_ref, v_ref, p_ref, o_ref, n_ref,
            wqkv, wo, w1, w2, sml, tok, n1s, h1, x0, x1, buf0, buf1, fl, st, s0, r0, s1, r1, local):
    i, last = pl.program_id(0), s.n // b - 1
    z = Sizes(n)
    place = Place(n)
    a, c = Gather(place, x0, buf0, s0, r0), Gather(place, x1, buf1, s1, r1)

    def norms(first, past):
        def one(u, _):
            r = pl.multiple_of(u * s.rows, s.rows)
            n1s[pl.ds(r + s.rows - 16, 16), :] = jnp.zeros((16, D), F32)
            n1s[pl.ds(r, s.len), :] = norm_fwd(tok[u].astype(F32))[0]
            return 0

        lax.fori_loop(first, past, one, 0)

    @pl.when(i == 0)
    def _():
        copy = pltpu.make_async_copy(x_hbm, tok, local)
        copy.start()
        zero(sml, st, x0, x1)
        st[0:1, :z.norm] = n_in[...].astype(F32)
        st[1:2, :z.bias] = b_in[...].astype(F32)
        x0[:z.q, :] = q_in[...]
        x0[z.small:z.small + 16, :] = st[:16, :].astype(BF16)
        x1[:z.o, :] = o_in[...]
        x1[z.f1:z.f1 + z.f, :] = f1_in[...]
        x1[z.f2:z.f2 + z.f, :] = f2_in[...]
        buf0[place.me] = x0[...]
        buf1[place.me] = x1[...]
        greet(place)
        a.begin()
        copy.wait()
        groups = levels(a.arrivals())
        for k, level in enumerate(groups):
            norms(k * s.n // len(groups), (k + 1) * s.n // len(groups))
            for h, off in groups[level]:
                a.arrive(h, off)
        a.finish()
        c.begin()
        unpack_small(z, buf0, sml)
        unpack(z, buf0, 0, z.q, fl, wqkv)

    rows = b * s.rows
    n1 = n1s[pl.ds(pl.multiple_of(i * rows, rows), rows), :]
    h1[...] = (n1 * vec(sml, 0) + vec(sml, 3)).astype(BF16)
    for u in range(b):
        n_ref[u] = n1[u * s.rows:(u + 1) * s.rows].astype(BF16)
    attn_fwd(s, b, h1, wqkv, sml, q_ref, k_ref, v_ref, p_ref, o_ref)

    for level, events in levels(c.arrivals()).items():
        @pl.when(i == min(2 * level, last))
        def _():
            for h, off in events:
                c.arrive(h, off)

    @pl.when(i == last)
    def _():
        c.finish()
        unpack(z, buf1, 0, z.o, fl, wo)
        unpack(z, buf1, z.f1, z.f, fl, w1)
        unpack(z, buf1, z.f2, z.f, fl, w2)


def call1(n, tokens, shards):
    s, z = Pad(tokens), Sizes(n)
    b = s.step(2)
    saved = [((s.lanes, D), BF16), ((s.rows, D), BF16), ((s.rows, D), BF16), ((PAIRS, s.rows, 2 * s.lanes), BF16), ((s.rows, D), BF16), ((s.rows, D), BF16)]
    whole = [((D, 3 * D), BF16), ((D, D), BF16), ((D, FF), BF16), ((FF, D), BF16), ((48, 128), F32)]
    return pl.pallas_call(
        functools.partial(kernel1, n, s, b), grid=(s.n // b,),
        in_specs=[pl.BlockSpec(memory_space=pl.ANY)] + [const(*v.shape) for v in shards],
        out_specs=[img(b, *v[0]) for v in saved] + [const(*v[0]) for v in whole],
        out_shape=[SDS((s.n,) + v[0], v[1]) for v in saved] + [SDS(*v) for v in whole],
        scratch_shapes=[VM((s.n, s.len, D), BF16), VM((s.n * s.rows, D), F32), VM((b * s.rows, D), BF16),
                        VM((z.r0, 128), BF16), VM((z.r1, 128), BF16), VM((n, z.r0, 128), BF16), VM((n, z.r1, 128), BF16),
                        VM((4608 + 16, 128), F32), VM((16, 128), F32)] + sems(n) + sems(n) + [pltpu.SemaphoreType.DMA],
        compiler_params=big(collective_id=0, has_side_effects=True))(tokens, *shards)


def kernel2(n, s, b, sb, ch, valid, x_ref, c_ref, o_ref, wo, w1, w2, sml, out_ref, gx_ref, go_ref, part, gsm,
            xp, cp, ch_, os_, n2s, r2s, h2s, as_, gzs, x1s, gxb, w1x, w2t, gout, gfc1, gfc2t, fl):
    i = pl.program_id(0)
    z = Sizes(n)
    rows = b * s.rows

    @pl.when(i == 0)
    def _():
        zero(xp, cp, gout, gfc1, gfc2t, gsm)
        for r in (os_, h2s, as_, gzs, gxb):
            pad = r.shape[0] - rows
            if pad:
                r[rows:, :] = jnp.zeros((pad, r.shape[1]), BF16)
        ffn_setup(s, b, w1, w2, sml, w1x, w2t, h2s)

    ffn(s, b, sb, ch, i, valid, x_ref, c_ref, o_ref, wo, w1x, w2, w2t, sml, out_ref, gx_ref, go_ref,
        gout, gfc1, gfc2t, gsm, xp, cp, ch_, os_, n2s, r2s, h2s, as_, gzs, x1s, gxb)

    @pl.when(i == s.n // b - 1)
    def _():
        zero(part)
        gsm[0:1, 7 * D:7 * D + FF] = gfc1[D:D + 1, :]
        flatten(gout, D, fl)
        pack(z, fl, z.o, 0, part)
        flatten(gfc1, D, fl)
        pack(z, fl, z.f, z.f1, part)
        for j in range(3):
            fl[pl.ds(j, FF, stride=3), :] = gfc2t[128 * j:128 * j + 128, :].T * RS2
        pack(z, fl, z.f, z.f2, part)


def call2(n, valid, tokens, cot, o, wo, w1, w2, sml):
    s, z = Pad(tokens), Sizes(n)
    b = s.step(6)
    sb = max(k for k in range(1, 4) if b % k == 0)
    rows = b * s.rows
    up, sr = -(-rows // 256) * 256, sb * s.rows
    grid_spec = pltpu.PrefetchScalarGridSpec(
        num_scalar_prefetch=1, grid=(s.n // b,),
        in_specs=[img(b, s.len, D), img(b, s.len, D), img(b, s.rows, D), const(D, D), const(D, FF), const(FF, D), const(48, 128)],
        out_specs=[img(b, s.len, D), img(b, s.rows, D), img(b, s.lanes, D), const(n, z.r1, 128), const(8, 8 * D + FF)],
        scratch_shapes=[VM((sr, D), BF16), VM((up, D), BF16), VM((sr, D), BF16), VM((up, D), BF16), VM((rows, D), F32), VM((rows, 1), F32),
                        VM((up, D + 128), BF16), VM((up, FF), BF16), VM((up, FF), BF16), VM((rows, D), F32), VM((up, D), BF16),
                        VM((D + 128, FF), BF16), VM((D, FF), BF16), VM((D, D), F32), VM((D + 16, FF), F32), VM((D, FF), F32),
                        VM((4608 + 16, 128), F32)])
    return pl.pallas_call(
        functools.partial(kernel2, n, s, b, sb, 256), grid_spec=grid_spec,
        out_shape=[SDS(tokens.shape, BF16), SDS((s.n, s.rows, D), BF16), SDS((s.n, s.lanes, D), BF16),
                   SDS((n, z.r1, 128), BF16), SDS((8, 8 * D + FF), F32)],
        compiler_params=big())(valid, tokens, cot, o, wo, w1, w2, sml)


def kernel3(n, s, b, q_ref, k_ref, v_ref, p_ref, go_ref, n_ref, wqkv, sml, gsm, part_in, gt_ref, part0, res,
            part, rc, rb, nacc, gcs, n1b, gts, fl, s1, r1, local):
    i, last = pl.program_id(0), s.n // b - 1
    z = Sizes(n)
    place = Place(n)
    r = Reduce(place, part, rc, rb, s1, r1)

    @pl.when(i == 0)
    def _():
        copy = pltpu.make_async_copy(part_in, part, local)
        copy.start()
        zero(nacc, gcs)
        greet(place)
        copy.wait()
        r.begin()

    attn_bwd(s, b, q_ref, k_ref, v_ref, p_ref, go_ref, gt_ref, gts, gcs)
    for u in range(b):
        n1b[u * s.rows:(u + 1) * s.rows, :] = n_ref[u]
    nacc[...] += tn(n1b[...], gts[...])

    @pl.when(i == last)
    def _():
        zero(part0)
        finish_qkv(z, nacc, gcs, wqkv, sml, gsm, fl, part0)

    for level, events in levels(r.order()).items():
        @pl.when(i == min(2 + 2 * (3 - level), last))
        def _():
            for h, off in events:
                acc = r.advance(h, off)
                if not any(off):
                    res[r.rows(h), :] = acc

    @pl.when(i == last)
    def _():
        r.finish()


def call3(n, s, q, k, v, p, go, n1, wqkv, sml, gsm, part):
    z = Sizes(n)
    b = s.step(2)
    c, rows = n // 2, b * s.rows
    return pl.pallas_call(
        functools.partial(kernel3, n, s, b), grid=(s.n // b,),
        in_specs=[img(b, s.lanes, D), img(b, s.rows, D), img(b, s.rows, D), img(b, PAIRS, s.rows, 2 * s.lanes), img(b, s.lanes, D),
                  img(b, s.rows, D), const(D, 3 * D), const(48, 128), const(8, 8 * D + FF), pl.BlockSpec(memory_space=pl.ANY)],
        out_specs=[img(b, s.rows, 3 * D), const(n, z.r0, 128), const(z.r1, 128)],
        out_shape=[SDS((s.n, s.rows, 3 * D), BF16), SDS((n, z.r0, 128), BF16), SDS((z.r1, 128), F32)],
        scratch_shapes=[VM((n, z.r1, 128), BF16), VM((c, z.r1, 128), BF16), VM((c, z.r1, 128), BF16),
                        VM((D, 3 * D), F32), VM((8, 3 * D), F32), VM((rows, D), BF16), VM((rows, 3 * D), BF16),
                        VM((3456 + 16, 128), F32)] + sems(n) + [pltpu.SemaphoreType.DMA],
        compiler_params=big(collective_id=1, has_side_effects=True))(q, k, v, p, go, n1, wqkv, sml, gsm, part)


def kernel4(n, s, b, x_ref, gt_ref, gx_ref, wqkv, sml, part_in, dx_ref, res, part, rc, rb, xp, gts, s0, r0, local):
    i, last = pl.program_id(0), s.n // b - 1
    place = Place(n)
    r = Reduce(place, part, rc, rb, s0, r0)

    @pl.when(i == 0)
    def _():
        copy = pltpu.make_async_copy(part_in, part, local)
        copy.start()
        zero(xp)
        greet(place)
        copy.wait()
        r.begin()

    proj_bwd(s, b, x_ref, gt_ref, gx_ref, wqkv, sml, dx_ref, xp, gts)

    for level, events in levels(r.order()).items():
        @pl.when(i == min(1 + 2 * (3 - level), last))
        def _():
            for h, off in events:
                acc = r.advance(h, off)
                if not any(off):
                    res[r.rows(h), :] = acc

    @pl.when(i == last)
    def _():
        r.finish()


def call4(n, tokens, gt, gx, wqkv, sml, part):
    s, z = Pad(tokens), Sizes(n)
    b = s.step(2)
    c, rows = n // 2, b * s.rows
    return pl.pallas_call(
        functools.partial(kernel4, n, s, b), grid=(s.n // b,),
        in_specs=[img(b, s.len, D), img(b, s.rows, 3 * D), img(b, s.rows, D), const(D, 3 * D), const(48, 128), pl.BlockSpec(memory_space=pl.ANY)],
        out_specs=[img(b, s.len, D), const(z.r0, 128)],
        out_shape=[SDS(tokens.shape, BF16), SDS((z.r0, 128), F32)],
        scratch_shapes=[VM((n, z.r0, 128), BF16), VM((c, z.r0, 128), BF16), VM((c, z.r0, 128), BF16),
                        VM((rows, D), BF16), VM((rows, 3 * D), BF16)] + sems(n) + [pltpu.SemaphoreType.DMA],
        compiler_params=big(collective_id=2, has_side_effects=True))(tokens, gt, gx, wqkv, sml, part)


def kernel5(n, dx_in, res0, res1, dx, oq, oo, o1, o2, on, ob):
    z = Sizes(n)
    dx[...] = dx_in[...].astype(F32)

    @pl.when(pl.program_id(0) == 0)
    def _():
        oq[...] = res0[:z.q, :]
        on[...] = res0[z.small:z.small + 1, :z.norm]
        ob[...] = res0[z.small + 1:z.small + 2, :z.bias]
        oo[...] = res1[:z.o, :]
        o1[...] = res1[z.f1:z.f1 + z.f, :]
        o2[...] = res1[z.f2:z.f2 + z.f, :]


def call5(n, dx, res0, res1):
    s, z = Pad(dx), Sizes(n)
    b = s.step(3)
    shapes = [(z.q, 128), (z.o, 128), (z.f, 128), (z.f, 128), (1, z.norm), (1, z.bias)]
    return pl.pallas_call(
        functools.partial(kernel5, n), grid=(s.n // b,),
        in_specs=[img(b, s.len, D), const(z.r0, 128), const(z.r1, 128)],
        out_specs=[img(b, s.len, D)] + [const(*v) for v in shapes],
        out_shape=[SDS(dx.shape, F32)] + [SDS(v, F32) for v in shapes],
        compiler_params=big())(dx, res0, res1)


def local(n, tokens, cotangent, valid_slots, qkv_weight, out_weight, fc1_weight, fc2_weight, norm_params, bias_params):
    shards = [v.reshape(-1, 128) for v in (qkv_weight, out_weight, fc1_weight, fc2_weight)]
    shards += [norm_params.reshape(1, -1), bias_params.reshape(1, -1)]
    s = Pad(tokens)
    q, k, v, p, o, n1, wqkv, wo, w1, w2, sml = call1(n, tokens, shards)
    out, gx, go, part1, gsm = call2(n, valid_slots, tokens, cotangent, o, wo, w1, w2, sml)
    gt, part0, res1 = call3(n, s, q, k, v, p, go, n1, wqkv, sml, gsm, part1)
    dx, res0 = call4(n, tokens, gt, gx, wqkv, sml, part0)
    dx, *grads = call5(n, dx, res0, res1)
    return (out, dx) + tuple(v.reshape(-1) for v in grads)


def solution(mesh):
    s3, s1 = P("dev", None, None), P("dev")
    return jax.shard_map(functools.partial(local, mesh.shape["dev"]), mesh=mesh, in_specs=(s3, s3) + (s1,) * 7,
                         out_specs=(s3, s3) + (s1,) * 6, check_vma=False)
```

```python
import functools
import jax
import jax.numpy as jnp
from jax import lax
from jax.experimental import pallas as pl
from jax.experimental.pallas import tpu as pltpu
from jax.sharding import PartitionSpec as P

D, HEADS, HEAD_DIM, FF = 384, 6, 64, 1536
PAIRS = HEADS // 2
EPS = 1e-6
F32, BF16 = jnp.float32, jnp.bfloat16
RS2 = 0.7071067811865476
RS2PI = 0.3989422804014327
VM = pltpu.VMEM
BIAS_ROW = 16
SDS = jax.ShapeDtypeStruct


def nn(a, b):
    return lax.dot_general(a, b, (((1,), (0,)), ((), ())), preferred_element_type=F32)


def nt(a, b):
    return lax.dot_general(a, b, (((1,), (1,)), ((), ())), preferred_element_type=F32)


def tn(a, b):
    return lax.dot_general(a, b, (((0,), (0,)), ((), ())), preferred_element_type=F32)


def col8(v):
    return v.reshape(v.shape[0] // 8, 8, v.shape[1]).sum(axis=0)


def norm_fwd(v):
    c = v - jnp.mean(v, axis=1, keepdims=True)
    r = lax.rsqrt(jnp.mean(c * c, axis=1, keepdims=True) + EPS)
    return c * r, r


def norm_bwd(g, n, r, gain):
    e = g * gain
    return r * (e - jnp.mean(e, axis=1, keepdims=True) - n * jnp.mean(e * n, axis=1, keepdims=True))


def vec(sml, row, count=3):
    return jnp.concatenate([sml[row + j:row + j + 1, :] for j in range(count)], axis=1)


def low_lanes():
    return lax.broadcasted_iota(jnp.int32, (1, 128), 1) < 64


def stacked(v):
    low, z = low_lanes(), jnp.zeros_like(v)
    return jnp.concatenate([jnp.where(low, v, z), jnp.where(low, z, v)], axis=0)


class Pad:
    def __init__(self, tokens):
        self.n, self.len, _ = tokens.shape
        self.rows = -(-self.len // 16) * 16
        self.lanes = -(-self.len // 128) * 128

    def step(self, most):
        return max(b for b in range(1, most + 1) if self.n % b == 0)


def staged(items, *stages):
    held = {}
    for tick in range(len(items) + len(stages) - 1):
        for j in range(len(stages)):
            k = tick - j
            if 0 <= k < len(items):
                held[k] = stages[j](items[k], held.get(k))


def attn_fwd(s, b, h1, wqkv, sml, q_ref, k_ref, v_ref, p_ref, o_ref):
    lp, qp, low = s.rows, s.lanes, low_lanes()
    t = nn(h1[...], wqkv[...])
    q = (t[:, :D] + vec(sml, BIAS_ROW)).astype(BF16) * BF16(0.125)
    k = t[:, D:2 * D].astype(BF16)
    v = (t[:, 2 * D:] + vec(sml, BIAS_ROW + 3)).astype(BF16)
    for u in range(b):
        rows = slice(u * lp, u * lp + lp)
        q_ref[u, :lp, :] = q[rows]
        q_ref[u, lp:, :] = jnp.zeros((qp - lp, D), BF16)
        k_ref[u] = k[rows]
        v_ref[u] = v[rows]

    def scores(item, _):
        u, j = item
        cols = slice(128 * j, 128 * j + 128)
        return nt(k_ref[u, :, cols], stacked(q_ref[u, :, cols]))

    def softmax(item, st):
        u, j = item
        cols = slice(128 * j, 128 * j + 128)
        top, bot = st[:lp - 16], st[lp - 16:]
        row = lax.broadcasted_iota(jnp.int32, bot.shape, 0) + (lp - 16)
        bot = jnp.where(row < s.len, bot, -1e30)
        mx = jnp.maximum(jnp.max(top, axis=0, keepdims=True), jnp.max(bot, axis=0, keepdims=True))
        e = jnp.exp(jnp.concatenate([top, bot], axis=0) - mx)
        p = (e * (1.0 / jnp.sum(e, axis=0, keepdims=True))).astype(BF16)
        p_ref[u, j] = p

    def mix(item, _):
        u, j = item
        cols = slice(128 * j, 128 * j + 128)
        p, v = p_ref[u, j], v_ref[u, :, cols]
        o_ref[u, :, cols] = jnp.where(low, tn(p[:, :lp], v), tn(p[:, qp:qp + lp], v)).astype(BF16)

    staged([(u, j) for u in range(b) for j in range(PAIRS)], scores, softmax, mix)


def attn_bwd(s, b, q_ref, k_ref, v_ref, p_ref, go_ref, gt_ref, gts, gcs):
    lp, qp, low = s.rows, s.lanes, low_lanes()

    def first(item, _):
        u, j = item
        cols = slice(128 * j, 128 * j + 128)
        p, go = p_ref[u, j], go_ref[u, :, cols]
        gp = nt(v_ref[u, :, cols], stacked(go))
        gv = jnp.where(low, nn(p[:, :qp], go), nn(p[:, qp:], go))
        return gp, gv

    def middle(item, got):
        u, j = item
        gp, gv = got
        pf = p_ref[u, j].astype(F32)
        return (pf * (gp - jnp.sum(gp * pf, axis=0, keepdims=True))).astype(BF16), gv

    def rest(item, got):
        u, j = item
        gs, gv = got
        cols = slice(128 * j, 128 * j + 128)
        k, q = k_ref[u, :, cols], q_ref[u, :, cols]
        gq = jnp.where(low, tn(gs[:, :lp], k), tn(gs[:, qp:qp + lp], k)) * 0.125
        gk = jnp.where(low, nn(gs[:, :qp], q), nn(gs[:, qp:], q))
        for part, g in enumerate((gq, gk, gv)):
            here = slice(part * D + 128 * j, part * D + 128 * j + 128)
            gcs[:, here] += col8(g)
            g = g.astype(BF16)
            gt_ref[u, :, here] = g
            gts[u * lp:u * lp + lp, here] = g

    staged([(u, j) for u in range(b) for j in range(PAIRS)], first, middle, rest)


LOG2E = 1.4426950408889634
LOG2_2C = 0.17425193526384086
ROOT2 = 1.4142135623730951


def ffn(s, b, sb, ch, i, valid, x_ref, c_ref, o_ref, wo, w1x, w2, w2t, sml,
        out_ref, gx_ref, go_ref, gout, gfc1, gfc2t, gsm, xp, cp, ch_, os_, n2s, r2s, h2s, as_, gzs, x1s, gxb):
    lp, qp = s.rows, s.lanes
    g2, c2 = vec(sml, 6), vec(sml, 9)
    bo, b2 = vec(sml, BIAS_ROW + 6), vec(sml, BIAS_ROW + 21)
    sr = sb * lp
    rows_all = b * lp

    def sub(t, _):
        for u in range(sb):
            w = t * sb + u
            m = valid[i * b + w].astype(BF16)
            xp[u * lp:u * lp + s.len, :] = x_ref[w]
            r0 = pl.multiple_of(w * lp, lp)
            cp[pl.ds(r0, s.len), :] = c_ref[w] * m
            os_[pl.ds(r0, lp), :] = o_ref[w]
        rows = pl.ds(pl.multiple_of(t * sr, sr), sr)
        x1 = xp[...].astype(F32) + nn(os_[rows, :], wo[...]) + bo
        x1s[rows, :] = x1
        n2, r2 = norm_fwd(x1)
        n2s[rows, :] = n2
        r2s[rows, :] = r2
        h2s[rows, :D] = (n2 * g2 + c2).astype(BF16)
        ch_[...] = cp[rows, :] * BF16(0.5)
        for c in range(FF // ch):
            cols = slice(c * ch, (c + 1) * ch)
            z = nn(h2s[rows, :], w1x[:, cols])
            ga = nt(ch_[...], w2[cols, :])
            w = z * RS2
            u1 = 1.0 + lax.erf(w)
            as_[rows, cols] = (w * u1).astype(BF16)
            gzs[rows, cols] = (ga * (u1 + w * jnp.exp2(w * w * -LOG2E + LOG2_2C))).astype(BF16)
        return 0

    lax.fori_loop(0, b // sb, sub, 0)
    yt = nt(w2t[...], as_[...])
    gt = nt(w1x[:D, :], gzs[...])
    y = yt.T[:rows_all] * RS2 + x1s[...] + b2
    for u in range(b):
        out_ref[u] = (y[u * lp:u * lp + s.len] * valid[i * b + u].astype(F32)).astype(BF16)
    gh2 = gt.T[:rows_all]
    n2 = n2s[...]
    gy = cp[:rows_all, :].astype(F32)
    gsm[:, 2 * D:3 * D] += col8(gh2 * n2)
    gsm[:, 3 * D:4 * D] += col8(gh2)
    gsm[:, 7 * D + FF:] += col8(gy)
    gx1 = gy + norm_bwd(gh2, n2, r2s[...], g2)
    gsm[:, 6 * D:7 * D] += col8(gx1)
    gxb[:rows_all, :] = gx1.astype(BF16)
    gfc2t[...] += tn(cp[...], as_[...])
    gfc1[...] += tn(h2s[:, :D + 16], gzs[...])
    gout[...] += tn(os_[...], gxb[...])
    go = nt(gxb[:rows_all, :], wo[...]).astype(BF16)
    for u in range(b):
        gx_ref[u] = gxb[u * lp:u * lp + lp, :]
        go_ref[u, :lp, :] = go[u * lp:u * lp + lp]
        go_ref[u, lp:, :] = jnp.zeros((qp - lp, D), BF16)


def ffn_setup(s, b, w1, w2, sml, w1x, w2t, h2s):
    w1x[:D, :] = w1[...]
    w1x[D:D + 16, :] = jnp.concatenate([vec(sml, BIAS_ROW + 9, 12), jnp.zeros((15, FF), F32)], axis=0).astype(BF16)
    w1x[D + 16:, :] = jnp.zeros((112, FF), BF16)
    w2t[...] = w2[...].T
    lane = lax.broadcasted_iota(jnp.int32, (b * s.rows, 128), 1)
    h2s[:b * s.rows, D:] = jnp.where(lane == 0, 1.0, 0.0).astype(BF16)


def proj_bwd(s, b, x_ref, gt_ref, gx_ref, wqkv, sml, dx_ref, xp, gts):
    lp = s.rows
    for u in range(b):
        xp[u * lp:u * lp + s.len, :] = x_ref[u]
        gts[u * lp:u * lp + lp, :] = gt_ref[u]
    n1, r1 = norm_fwd(xp[...].astype(F32))
    back = norm_bwd(nt(gts[...], wqkv[...]), n1, r1, vec(sml, 0))
    for u in range(b):
        dx_ref[u] = (gx_ref[u].astype(F32) + back[u * lp:u * lp + lp]).astype(BF16)[:s.len]


def zero(*refs):
    for r in refs:
        r[...] = jnp.zeros_like(r)


def img(b, *shape):
    return pl.BlockSpec((b,) + shape, lambda i, *_: (i,) + (0,) * len(shape))


def const(*shape):
    return pl.BlockSpec(shape, lambda i, *_: (0,) * len(shape), pipeline_mode=pl.Buffered(1))


def big(**kw):
    return pltpu.CompilerParams(vmem_limit_bytes=62 << 20, **kw)


MESHID = pl.DeviceIdType.MESH


def chip_dims(n):
    chips = n // 2
    side = 4 if chips >= 64 else 2
    return (chips // (side * side), side, side)


class Place:
    def __init__(self, n):
        self.n, self.dims = n, chip_dims(n)
        s0, s1, s2 = self.dims
        self.me = lax.axis_index("dev")
        self.core = lax.rem(self.me, 2)
        chip = self.me // 2
        at = (chip // (s1 * s2), lax.rem(chip // s2, s1), lax.rem(chip, s2))
        pitch = (2 * s1 * s2, 2 * s2, 2)
        self.term = [[(lax.rem(i + o, s) if o else i) * w for o in range(s)] for i, s, w in zip(at, self.dims, pitch)]
        self.offs = [(a, b, c) for a in range(s0) for b in range(s1) for c in range(s2)]
        base = {o: self.term[0][o[0]] + self.term[1][o[1]] + self.term[2][o[2]] for o in self.offs}
        self.same = {o: v + self.core for o, v in base.items()}
        self.other = {o: v + 1 - self.core for o, v in base.items()}

    def key(self, off):
        return tuple(o % s for o, s in zip(off, self.dims))

    def dev(self, off):
        return self.same[self.key(off)]

    def partner(self, off=(0, 0, 0)):
        return self.other[self.key(off)]

    def num(self, off):
        return (off[0] * self.dims[1] + off[1]) * self.dims[2] + off[2]

    def peers(self):
        for k in range(3):
            for o in range(1, self.dims[k]):
                yield self.dev(unit(k, o))
        yield self.partner()


def unit(k, o):
    return tuple(o if j == k else 0 for j in range(3))


def neg(off):
    return tuple(-o for o in off)


def greet(pl_):
    barrier = pltpu.get_barrier_semaphore()
    count = 0
    for dev in pl_.peers():
        pl.semaphore_signal(barrier, inc=1, device_id=(dev,), device_id_type=MESHID)
        count += 1
    pl.semaphore_wait(barrier, count)


ORDERS = ((0, 2, 1), (0, 1, 2))


def stage(h, off):
    return max([j for j in range(3) if off[ORDERS[h][j]]], default=-1)


class Gather:
    def __init__(self, place, src, buf, ssem, rsem):
        self.p, self.src, self.buf, self.ssem, self.rsem = place, src, buf, ssem, rsem
        self.half = src.shape[0] // 2

    def link(self, h, off, to, dev):
        p, rows = self.p, pl.ds(h * self.half, self.half)
        origin = p.dev(neg(off))
        src = self.src.at[rows] if not any(off) else self.buf.at[origin, rows]
        k = p.num(to)
        return pltpu.make_async_remote_copy(
            src_ref=src, dst_ref=self.buf.at[origin, rows], send_sem=self.ssem.at[0, h, k],
            recv_sem=self.rsem.at[0, h, k], device_id=(dev,), device_id_type=MESHID)

    def cross(self, h, off):
        p, rows = self.p, pl.ds(h * self.half, self.half)
        origin = p.dev(neg(off))
        src = self.src.at[rows] if not any(off) else self.buf.at[origin, rows]
        k = p.num(off)
        return pltpu.make_async_remote_copy(
            src_ref=src, dst_ref=self.buf.at[origin, rows], send_sem=self.ssem.at[1, h, k],
            recv_sem=self.rsem.at[1, h, k], device_id=(p.partner(),), device_id_type=MESHID)

    def hops(self, h, off):
        order = ORDERS[h]
        last = max([j for j in range(3) if off[order[j]]], default=-1)
        for j in range(last + 1, 3):
            k = order[j]
            for o in range(1, self.p.dims[k]):
                to = tuple(a + b for a, b in zip(off, unit(k, o)))
                yield to, self.p.dev(unit(k, o))

    def forward(self, h, off):
        for to, dev in self.hops(h, off):
            self.link(h, off, to, dev).start()
        self.cross(h, off).start()

    def begin(self):
        self.begin_first()
        self.begin_rest()

    def begin_first(self):
        for h in range(2):
            for to, dev in self.hops(h, (0, 0, 0)):
                if to[ORDERS[h][0]]:
                    self.link(h, (0, 0, 0), to, dev).start()

    def begin_rest(self):
        for h in range(2):
            for to, dev in self.hops(h, (0, 0, 0)):
                if not to[ORDERS[h][0]]:
                    self.link(h, (0, 0, 0), to, dev).start()
            self.cross(h, (0, 0, 0)).start()

    def arrivals(self):
        offs = sorted([o for o in self.p.offs if any(o)], key=lambda o: (sum(1 for a in o if a), min(o[0], self.p.dims[0] - o[0])))
        return [(h, o) for o in offs for h in range(2)]

    def arrive(self, h, off):
        self.link(h, off, off, self.p.me).wait_recv()
        self.forward(h, off)

    def finish(self):
        for h in range(2):
            for off in self.p.offs:
                c = self.cross(h, off)
                c.wait_recv()
                c.wait_send()
                for to, dev in self.hops(h, off):
                    self.link(h, off, to, dev).wait_send()


class Reduce:
    def __init__(self, place, part, rc, rb, ssem, rsem, key):
        self.key = key
        self.p, self.part, self.rc, self.rb, self.ssem, self.rsem = place, part, rc, rb, ssem, rsem
        self.half = part.shape[1] // 2

    def rows(self, h):
        return pl.ds(h * self.half, self.half)

    def cross(self, h, off):
        p, k = self.p, self.p.num(off)
        return pltpu.make_async_remote_copy(
            src_ref=self.part.at[p.partner(off), self.rows(h)], dst_ref=self.rc.at[k, self.rows(h)],
            send_sem=self.ssem.at[1, h, k], recv_sem=self.rsem.at[1, h, k],
            device_id=(p.partner(),), device_id_type=MESHID)

    def step_dim(self, h, off):
        return [k for k in reversed(ORDERS[h]) if off[k]][0]

    def link(self, h, off):
        p, k = self.p, self.p.num(off)
        dim = self.step_dim(h, off)
        return pltpu.make_async_remote_copy(
            src_ref=self.part.at[p.dev(off), self.rows(h)], dst_ref=self.rb.at[k, self.rows(h)],
            send_sem=self.ssem.at[0, h, k], recv_sem=self.rsem.at[0, h, k],
            device_id=(p.dev(unit(dim, off[dim])),), device_id_type=MESHID)

    def sources(self, h, off):
        order = ORDERS[h]
        last = max([j for j in range(3) if off[order[j]]], default=-1)
        for j in reversed(range(last + 1, 3)):
            k = order[j]
            for o in range(1, self.p.dims[k]):
                yield tuple(a + b for a, b in zip(off, unit(k, o)))

    def order(self):
        return sorted([(h, o) for o in self.p.offs for h in range(2)], key=lambda e: (-self.key(*e), e[1]))

    def begin(self):
        for h, off in self.order():
            self.cross(h, off).start()

    def total(self, h, off, first=0):
        p, k = self.p, self.p.num(off)
        self.cross(h, off).wait_recv()
        acc = self.part[p.dev(off), self.rows(h), :].astype(F32) + self.rc[k, self.rows(h), :].astype(F32)
        for s in self.sources(h, off):
            if stage(h, s) < first:
                continue
            self.link(h, s).wait_recv()
            acc += self.rb[p.num(s), self.rows(h), :].astype(F32)
        return acc

    def advance(self, h, off):
        acc = self.total(h, off)
        if any(off):
            self.part[self.p.dev(off), self.rows(h), :] = acc.astype(BF16)
            self.link(h, off).start()
        return acc

    def finish(self, first=0):
        for h, off in self.order():
            self.cross(h, off).wait_send()
            if stage(h, off) >= first:
                self.link(h, off).wait_send()


class Sizes:
    def __init__(self, n):
        up = lambda v, m: -(-v // m) * m
        self.n = n
        self.q, self.o, self.f = 3 * D * D // n // 128, D * D // n // 128, D * FF // n // 128
        self.norm, self.bias = 4 * D // n, (4 * D + FF) // n
        self.small = up(self.q, 16)
        self.r0 = up(self.small + 16, 32)
        self.f1 = up(self.o, 16)
        self.f2 = self.f1 + up(self.f, 16)
        self.r1 = up(self.f2 + up(self.f, 16), 32)


def sems(n):
    return [pltpu.SemaphoreType.DMA((2, 2, n // 2))] * 2


def count(h, off):
    return sum(1 for a in off if a)


def groups_by(key, events):
    groups = {}
    for h, off in events:
        groups.setdefault(key(h, off), []).append((h, off))
    return groups


AT_GATHER = {1: 2, 2: 5}
AT_FIRST = {2: 2, 1: 5}
AT_SECOND = {3: 1, 2: 3, 1: 5, 0: 7}


def at_step(i, k):
    return pl.when(i == k)


def unpack(z, buf, first, count, fl, w):
    def one(d, _):
        fl[pl.ds(d * count, count), :] = buf[d, first:first + -(-count // 16) * 16, :].astype(F32)[:count]
        return 0

    lax.fori_loop(0, z.n, one, 0)
    rows, cols = w.shape[0], w.shape[1] // 128
    for j in range(cols):
        w[:, 128 * j:128 * j + 128] = fl[pl.ds(j, rows, stride=cols), :].astype(BF16)


def unpack_small(z, buf, sml):
    lane = lax.broadcasted_iota(jnp.int32, (1, 128), 1)
    rows = {}

    def put(v, start, size):
        first, shift = divmod(start, 128)
        v = pltpu.roll(v, shift, axis=1) if shift else v
        cut = (lane >= shift) & (lane < shift + size)
        rows[first] = jnp.where(cut, v, rows.get(first, 0.0))
        if shift + size > 128:
            rows[first + 1] = jnp.where(lane < shift + size - 128, v, rows.get(first + 1, 0.0))

    for d in range(z.n):
        v = buf[d, z.small:z.small + 16, :].astype(F32)
        put(v[0:1], d * z.norm, z.norm)
        put(v[1:2], BIAS_ROW * 128 + d * z.bias, z.bias)
    for r, v in rows.items():
        sml[r:r + 1, :] = v


def flatten(g, rows, fl):
    cols = g.shape[1] // 128
    for j in range(cols):
        fl[pl.ds(j, rows, stride=cols), :] = g[:rows, 128 * j:128 * j + 128]


def pack(z, fl, count, first, part):
    size = -(-count // 16) * 16

    def one(d, _):
        part[d, first:first + size, :] = fl[pl.ds(d * count, size), :].astype(BF16)
        return 0

    lax.fori_loop(0, z.n, one, 0)


def column(row):
    return jnp.broadcast_to(row, (128, 128)).T


def finish_qkv(z, nacc, gcs, wqkv, sml, gsm, fl, part):
    total = jnp.sum(gcs[...], axis=0, keepdims=True)
    gain, shift = vec(sml, 0), vec(sml, 3)
    rows = {}
    for a in range(3):
        ra = slice(128 * a, 128 * a + 128)
        g, c = column(gain[:, ra]), column(shift[:, ra])
        q1, q2 = jnp.zeros((128, 128), F32), jnp.zeros((128, 128), F32)
        for j in range(9):
            cols = slice(128 * j, 128 * j + 128)
            na, w = nacc[ra, cols], wqkv[ra, cols].astype(F32)
            fl[pl.ds(9 * 128 * a + j, 128, stride=9), :] = g * na + c * total[:, cols]
            q1 += w * na
            q2 += w * total[:, cols]
        rows[a] = jnp.sum(q1.T, axis=0, keepdims=True)
        rows[3 + a] = jnp.sum(q2.T, axis=0, keepdims=True)
        rows[BIAS_ROW + a] = total[:, 128 * a:128 * a + 128]
        rows[BIAS_ROW + 3 + a] = total[:, 2 * D + 128 * a:2 * D + 128 * a + 128]

    def put(first, count, base):
        v = jnp.sum(gsm[:, first:first + 128 * count], axis=0, keepdims=True)
        for j in range(count):
            rows[base + j] = v[:, 128 * j:128 * j + 128]

    put(2 * D, 6, 6)
    put(6 * D, 18, BIAS_ROW + 6)
    pack(z, fl, z.q, 0, part)
    lane = lax.broadcasted_iota(jnp.int32, (1, 128), 1)

    def take(start, size):
        first, shift = divmod(start, 128)
        v = rows[first]
        if shift + size > 128:
            v = jnp.where(lane >= shift, v, rows[first + 1])
        return pltpu.roll(v, 128 - shift, axis=1) if shift else v

    for d in range(z.n):
        both = [take(d * z.norm, z.norm), take(BIAS_ROW * 128 + d * z.bias, z.bias)]
        part[d, z.small:z.small + 16, :] = jnp.concatenate(both + [jnp.zeros((14, 128), F32)], axis=0).astype(BF16)


def kernel1(n, s, b, x_hbm, q_in, o_in, f1_in, f2_in, n_in, b_in, q_ref, k_ref, v_ref, p_ref, o_ref, n_ref,
            wqkv, wo, w1, w2, sml, tok, n1s, h1, x0, x1, buf0, buf1, fl, st, s0, r0, s1, r1, local):
    i, last = pl.program_id(0), s.n // b - 1
    z = Sizes(n)
    place = Place(n)
    a, c = Gather(place, x0, buf0, s0, r0), Gather(place, x1, buf1, s1, r1)

    def norms(first, past):
        def one(u, _):
            r = pl.multiple_of(u * s.rows, s.rows)
            n1s[pl.ds(r + s.rows - 16, 16), :] = jnp.zeros((16, D), F32)
            n1s[pl.ds(r, s.len), :] = norm_fwd(tok[u].astype(F32))[0]
            return 0

        lax.fori_loop(first, past, one, 0)

    @pl.when(i == 0)
    def _():
        copy = pltpu.make_async_copy(x_hbm, tok, local)
        copy.start()
        zero(sml, st, x0, x1)
        st[0:1, :z.norm] = n_in[...].astype(F32)
        st[1:2, :z.bias] = b_in[...].astype(F32)
        x0[:z.q, :] = q_in[...]
        x0[z.small:z.small + 16, :] = st[:16, :].astype(BF16)
        x1[:z.o, :] = o_in[...]
        x1[z.f1:z.f1 + z.f, :] = f1_in[...]
        x1[z.f2:z.f2 + z.f, :] = f2_in[...]
        buf0[place.me] = x0[...]
        buf1[place.me] = x1[...]
        greet(place)
        a.begin()
        c.begin_first()
        copy.wait()
        groups = groups_by(count, a.arrivals())
        for k, level in enumerate(groups):
            norms(k * s.n // len(groups), (k + 1) * s.n // len(groups))
            for h, off in groups[level]:
                a.arrive(h, off)
        a.finish()
        c.begin_rest()
        unpack_small(z, buf0, sml)
        unpack(z, buf0, 0, z.q, fl, wqkv)
        for h, off in groups_by(stage, c.arrivals())[0]:
            c.arrive(h, off)

    rows = b * s.rows
    n1 = n1s[pl.ds(pl.multiple_of(i * rows, rows), rows), :]
    h1[...] = (n1 * vec(sml, 0) + vec(sml, 3)).astype(BF16)
    for u in range(b):
        n_ref[u] = n1[u * s.rows:(u + 1) * s.rows].astype(BF16)
    attn_fwd(s, b, h1, wqkv, sml, q_ref, k_ref, v_ref, p_ref, o_ref)

    for leg in (1, 2):
        events = groups_by(stage, c.arrivals())[leg]

        @pl.when(i == min(AT_GATHER[leg], last))
        def _():
            for h, off in events:
                c.arrive(h, off)

    @pl.when(i == last)
    def _():
        c.finish()
        unpack(z, buf1, 0, z.o, fl, wo)
        unpack(z, buf1, z.f1, z.f, fl, w1)
        unpack(z, buf1, z.f2, z.f, fl, w2)


def call1(n, tokens, shards):
    s, z = Pad(tokens), Sizes(n)
    b = s.step(2)
    saved = [((s.lanes, D), BF16), ((s.rows, D), BF16), ((s.rows, D), BF16), ((PAIRS, s.rows, 2 * s.lanes), BF16), ((s.rows, D), BF16), ((s.rows, D), BF16)]
    whole = [((D, 3 * D), BF16), ((D, D), BF16), ((D, FF), BF16), ((FF, D), BF16), ((48, 128), F32)]
    return pl.pallas_call(
        functools.partial(kernel1, n, s, b), grid=(s.n // b,),
        in_specs=[pl.BlockSpec(memory_space=pl.ANY)] + [const(*v.shape) for v in shards],
        out_specs=[img(b, *v[0]) for v in saved] + [const(*v[0]) for v in whole],
        out_shape=[SDS((s.n,) + v[0], v[1]) for v in saved] + [SDS(*v) for v in whole],
        scratch_shapes=[VM((s.n, s.len, D), BF16), VM((s.n * s.rows, D), F32), VM((b * s.rows, D), BF16),
                        VM((z.r0, 128), BF16), VM((z.r1, 128), BF16), VM((n, z.r0, 128), BF16), VM((n, z.r1, 128), BF16),
                        VM((4608 + 16, 128), F32), VM((16, 128), F32)] + sems(n) + sems(n) + [pltpu.SemaphoreType.DMA],
        compiler_params=big(collective_id=0, has_side_effects=True))(tokens, *shards)


def kernel2(n, s, b, sb, ch, valid, x_ref, c_ref, o_ref, wo, w1, w2, sml, out_ref, gx_ref, go_ref, part, gsm,
            xp, cp, ch_, os_, n2s, r2s, h2s, as_, gzs, x1s, gxb, w1x, w2t, gout, gfc1, gfc2t, fl):
    i = pl.program_id(0)
    z = Sizes(n)
    rows = b * s.rows

    @pl.when(i == 0)
    def _():
        zero(xp, cp, gout, gfc1, gfc2t, gsm)
        for r in (os_, h2s, as_, gzs, gxb):
            pad = r.shape[0] - rows
            if pad:
                r[rows:, :] = jnp.zeros((pad, r.shape[1]), BF16)
        ffn_setup(s, b, w1, w2, sml, w1x, w2t, h2s)

    ffn(s, b, sb, ch, i, valid, x_ref, c_ref, o_ref, wo, w1x, w2, w2t, sml, out_ref, gx_ref, go_ref,
        gout, gfc1, gfc2t, gsm, xp, cp, ch_, os_, n2s, r2s, h2s, as_, gzs, x1s, gxb)

    @pl.when(i == s.n // b - 1)
    def _():
        zero(part)
        gsm[0:1, 7 * D:7 * D + FF] = gfc1[D:D + 1, :]
        flatten(gout, D, fl)
        pack(z, fl, z.o, 0, part)
        flatten(gfc1, D, fl)
        pack(z, fl, z.f, z.f1, part)
        for j in range(3):
            fl[pl.ds(j, FF, stride=3), :] = gfc2t[128 * j:128 * j + 128, :].T * RS2
        pack(z, fl, z.f, z.f2, part)


def call2(n, valid, tokens, cot, o, wo, w1, w2, sml):
    s, z = Pad(tokens), Sizes(n)
    b = s.step(6)
    sb = max(k for k in range(1, 4) if b % k == 0)
    rows = b * s.rows
    up, sr = -(-rows // 256) * 256, sb * s.rows
    grid_spec = pltpu.PrefetchScalarGridSpec(
        num_scalar_prefetch=1, grid=(s.n // b,),
        in_specs=[img(b, s.len, D), img(b, s.len, D), img(b, s.rows, D), const(D, D), const(D, FF), const(FF, D), const(48, 128)],
        out_specs=[img(b, s.len, D), img(b, s.rows, D), img(b, s.lanes, D), const(n, z.r1, 128), const(8, 8 * D + FF)],
        scratch_shapes=[VM((sr, D), BF16), VM((up, D), BF16), VM((sr, D), BF16), VM((up, D), BF16), VM((rows, D), F32), VM((rows, 1), F32),
                        VM((up, D + 128), BF16), VM((up, FF), BF16), VM((up, FF), BF16), VM((rows, D), F32), VM((up, D), BF16),
                        VM((D + 128, FF), BF16), VM((D, FF), BF16), VM((D, D), F32), VM((D + 16, FF), F32), VM((D, FF), F32),
                        VM((4608 + 16, 128), F32)])
    return pl.pallas_call(
        functools.partial(kernel2, n, s, b, sb, 256), grid_spec=grid_spec,
        out_shape=[SDS(tokens.shape, BF16), SDS((s.n, s.rows, D), BF16), SDS((s.n, s.lanes, D), BF16),
                   SDS((n, z.r1, 128), BF16), SDS((8, 8 * D + FF), F32)],
        compiler_params=big())(valid, tokens, cot, o, wo, w1, w2, sml)


def kernel3(n, s, b, q_ref, k_ref, v_ref, p_ref, go_ref, n_ref, wqkv, sml, gsm, part_in, gt_ref, part0, mid,
            part, rc, rb, nacc, gcs, n1b, gts, fl, s1, r1, local):
    i, last = pl.program_id(0), s.n // b - 1
    z = Sizes(n)
    place = Place(n)
    r = Reduce(place, part, rc, rb, s1, r1, stage)

    @pl.when(i == 0)
    def _():
        copy = pltpu.make_async_copy(part_in, part, local)
        copy.start()
        zero(nacc, gcs)
        greet(place)
        copy.wait()
        r.begin()

    attn_bwd(s, b, q_ref, k_ref, v_ref, p_ref, go_ref, gt_ref, gts, gcs)
    for u in range(b):
        n1b[u * s.rows:(u + 1) * s.rows, :] = n_ref[u]
    nacc[...] += tn(n1b[...], gts[...])

    @pl.when(i == last)
    def _():
        zero(part0)
        finish_qkv(z, nacc, gcs, wqkv, sml, gsm, fl, part0)

    legs = groups_by(stage, r.order())
    for leg in (2, 1):
        @pl.when(i == min(AT_FIRST[leg], last))
        def _():
            for h, off in legs[leg]:
                r.advance(h, off)

    @pl.when(i == last)
    def _():
        for h, off in legs[0] + legs[-1]:
            mid[off[0], r.rows(h), :] = r.total(h, off, 1).astype(BF16)
        r.finish(1)


def call3(n, s, q, k, v, p, go, n1, wqkv, sml, gsm, part):
    z = Sizes(n)
    b = s.step(2)
    c, rows = n // 2, b * s.rows
    return pl.pallas_call(
        functools.partial(kernel3, n, s, b), grid=(s.n // b,),
        in_specs=[img(b, s.lanes, D), img(b, s.rows, D), img(b, s.rows, D), img(b, PAIRS, s.rows, 2 * s.lanes), img(b, s.lanes, D),
                  img(b, s.rows, D), const(D, 3 * D), const(48, 128), const(8, 8 * D + FF), pl.BlockSpec(memory_space=pl.ANY)],
        out_specs=[img(b, s.rows, 3 * D), const(n, z.r0, 128), const(chip_dims(n)[0], z.r1, 128)],
        out_shape=[SDS((s.n, s.rows, 3 * D), BF16), SDS((n, z.r0, 128), BF16), SDS((chip_dims(n)[0], z.r1, 128), BF16)],
        scratch_shapes=[VM((n, z.r1, 128), BF16), VM((c, z.r1, 128), BF16), VM((c, z.r1, 128), BF16),
                        VM((D, 3 * D), F32), VM((8, 3 * D), F32), VM((rows, D), BF16), VM((rows, 3 * D), BF16),
                        VM((3456 + 16, 128), F32)] + sems(n) + [pltpu.SemaphoreType.DMA],
        compiler_params=big(collective_id=1, has_side_effects=True))(q, k, v, p, go, n1, wqkv, sml, gsm, part)


def kernel4(n, s, b, x_ref, gt_ref, gx_ref, wqkv, sml, part_in, mid_in, dx_ref, res, res1,
            part, rc, rb, mid, rz, xp, gts, s0, r0, sz, qz, local):
    i, last = pl.program_id(0), s.n // b - 1
    place = Place(n)
    r = Reduce(place, part, rc, rb, s0, r0, count)
    far = range(1, place.dims[0])

    def along(o):
        return pltpu.make_async_remote_copy(
            src_ref=mid.at[o], dst_ref=rz.at[o], send_sem=sz.at[o], recv_sem=qz.at[o],
            device_id=(place.dev((o, 0, 0)),), device_id_type=MESHID)

    @pl.when(i == 0)
    def _():
        copies = [pltpu.make_async_copy(part_in, part, local.at[0]), pltpu.make_async_copy(mid_in, mid, local.at[1])]
        for copy in copies:
            copy.start()
        zero(xp)
        greet(place)
        for copy in copies:
            copy.wait()
        r.begin()
        for o in far:
            along(o).start()

    proj_bwd(s, b, x_ref, gt_ref, gx_ref, wqkv, sml, dx_ref, xp, gts)

    for level, events in groups_by(count, r.order()).items():
        @pl.when(i == min(AT_SECOND[level], last))
        def _():
            for h, off in events:
                acc = r.advance(h, off)
                if not any(off):
                    res[r.rows(h), :] = acc

    @pl.when(i == last)
    def _():
        acc = mid[0].astype(F32)
        for o in far:
            along(o).wait_recv()
            acc += rz[o].astype(F32)
        res1[...] = acc
        for o in far:
            along(o).wait_send()
        r.finish()


def call4(n, tokens, gt, gx, wqkv, sml, part, mid):
    s, z = Pad(tokens), Sizes(n)
    b = s.step(2)
    c, rows = n // 2, b * s.rows
    return pl.pallas_call(
        functools.partial(kernel4, n, s, b), grid=(s.n // b,),
        in_specs=[img(b, s.len, D), img(b, s.rows, 3 * D), img(b, s.rows, D), const(D, 3 * D), const(48, 128)] + [pl.BlockSpec(memory_space=pl.ANY)] * 2,
        out_specs=[img(b, s.len, D), const(z.r0, 128), const(z.r1, 128)],
        out_shape=[SDS(tokens.shape, BF16), SDS((z.r0, 128), F32), SDS((z.r1, 128), F32)],
        scratch_shapes=[VM((n, z.r0, 128), BF16), VM((c, z.r0, 128), BF16), VM((c, z.r0, 128), BF16),
                        VM(mid.shape, BF16), VM(mid.shape, BF16),
                        VM((rows, D), BF16), VM((rows, 3 * D), BF16)] + sems(n)
                       + [pltpu.SemaphoreType.DMA(mid.shape[:1])] * 2 + [pltpu.SemaphoreType.DMA((2,))],
        compiler_params=big(collective_id=2, has_side_effects=True))(tokens, gt, gx, wqkv, sml, part, mid)


def kernel5(n, dx_in, res0, res1, dx, oq, oo, o1, o2, on, ob):
    z = Sizes(n)
    dx[...] = dx_in[...].astype(F32)

    @pl.when(pl.program_id(0) == 0)
    def _():
        oq[...] = res0[:z.q, :]
        on[...] = res0[z.small:z.small + 1, :z.norm]
        ob[...] = res0[z.small + 1:z.small + 2, :z.bias]
        oo[...] = res1[:z.o, :]
        o1[...] = res1[z.f1:z.f1 + z.f, :]
        o2[...] = res1[z.f2:z.f2 + z.f, :]


def call5(n, dx, res0, res1):
    s, z = Pad(dx), Sizes(n)
    b = s.step(3)
    shapes = [(z.q, 128), (z.o, 128), (z.f, 128), (z.f, 128), (1, z.norm), (1, z.bias)]
    return pl.pallas_call(
        functools.partial(kernel5, n), grid=(s.n // b,),
        in_specs=[img(b, s.len, D), const(z.r0, 128), const(z.r1, 128)],
        out_specs=[img(b, s.len, D)] + [const(*v) for v in shapes],
        out_shape=[SDS(dx.shape, F32)] + [SDS(v, F32) for v in shapes],
        compiler_params=big())(dx, res0, res1)


def local(n, tokens, cotangent, valid_slots, qkv_weight, out_weight, fc1_weight, fc2_weight, norm_params, bias_params):
    shards = [v.reshape(-1, 128) for v in (qkv_weight, out_weight, fc1_weight, fc2_weight)]
    shards += [norm_params.reshape(1, -1), bias_params.reshape(1, -1)]
    s = Pad(tokens)
    q, k, v, p, o, n1, wqkv, wo, w1, w2, sml = call1(n, tokens, shards)
    out, gx, go, part1, gsm = call2(n, valid_slots, tokens, cotangent, o, wo, w1, w2, sml)
    gt, part0, mid = call3(n, s, q, k, v, p, go, n1, wqkv, sml, gsm, part1)
    dx, res0, res1 = call4(n, tokens, gt, gx, wqkv, sml, part0, mid)
    dx, *grads = call5(n, dx, res0, res1)
    return (out, dx) + tuple(v.reshape(-1) for v in grads)


def solution(mesh):
    s3, s1 = P("dev", None, None), P("dev")
    return jax.shard_map(functools.partial(local, mesh.shape["dev"]), mesh=mesh, in_specs=(s3, s3) + (s1,) * 7,
                         out_specs=(s3, s3) + (s1,) * 6, check_vma=False)
```
